256 devices in a mesh: seq: 64 (over x, y, z_hi), chan: 4 (over z_lo, core).
Axes of the slice: x: 4, y: 4, z: 8 (z_hi: 4, z_lo: 2; z = z_hi * 2 + z_lo), core: 2. Of those that a mesh axis runs over, the one named last changes fastest.
Arguments:
- tokens: bfloat16 [768, 131072], P('chan', 'seq'), may hold values from -7.5 to 7.5
- filter_spectrum: float32 [2, 768, 131072], P(None, 'chan', 'seq'), may hold values from -6 to 6
- skip_weight: float32 [768], P('chan'), may hold values from -1 to 1
- norm_gain: float32 [768], P('chan'), may hold values from 0.5 to 1.5
- mlp_gain: float32 [768], P('chan'), may hold values from 0.5 to 1.5
- mix_in: bfloat16 [4, 36864], P('chan'), may hold values from -0.4375 to 0.4375
- up_weight: bfloat16 [4, 147456], P('chan'), may hold values from -0.4375 to 0.4375
- down_weight: bfloat16 [4, 147456], P('chan'), may hold values from -0.21875 to 0.21875
- mix_out: bfloat16 [4, 36864], P('chan'), may hold values from -0.4375 to 0.4375
Outputs:
- mixed: bfloat16 [768, 131072], P('chan', 'seq')
The draws below stay inside these ranges and needn't reach their ends.
All inputs are finite; a program needn't handle non-finite values.
Results may differ from the reference program's by a relative error of at most 0.013.
Values may be sent and summed in bfloat16 or wider, within the bound.
No kernel may reach another device: no remote copies, remote signals or barrier semaphores. Data moves between devices by JAX's collectives and lax.ppermute only.
A program may use at most 64 MiB of HBM per device.

```python
import math
import jax
import jax.numpy as jnp
from jax import lax

D = 768
FF = 3072
BLOCKS = 4
RADIX = 64
TOK_DEV = 2048
TOKENS = 131072
N_SEQ = 64


def draw_tokens(key, part):
    noise_key, col_key = jax.random.split(key)
    channel = jnp.arange(D, dtype=jnp.float32) / D
    scales = 0.1 * 10.0 ** channel
    col_scale = 0.25 * 10.0 ** jax.random.uniform(col_key, (1, TOKENS), jnp.float32)
    values = jax.random.truncated_normal(noise_key, -3.0, 3.0, (D, TOKENS), jnp.float32)
    return (values * scales[:, None] * col_scale).astype(jnp.bfloat16)


def level_of(own_key, shape, pieces, low, largest):
    gain = 1.0
    for dim, blocks in pieces:
        heights = jax.random.uniform(jax.random.fold_in(jax.random.fold_in(own_key, 6), dim), (blocks,), jnp.float32, low / len(pieces), largest / len(pieces))
        gain = gain * jnp.repeat(jnp.exp(heights), shape[dim] // blocks).reshape((-1,) + (1,) * (len(shape) - 1 - dim))
    return gain


def centred(own_key, shape, spread, most, cuts=(), held_as=jnp.bfloat16):
    array = spread * jax.random.normal(own_key, shape, jnp.float32)
    if cuts:
        array = array * level_of(own_key, shape, cuts, -0.22, 0.18)
    return jnp.clip(array, -most, most).astype(held_as)


def setup_inputs(seed: int = 0) -> dict:
    streams_of = jax.random.split(jax.random.key(seed), 10)
    return {
        "tokens": draw_tokens(jax.random.fold_in(streams_of[9], 71), 0),
        "filter_spectrum": centred(streams_of[1], (2, D, TOKENS), 1.0, 6.0, ((1, 4), (2, 64)), jnp.float32),
        "skip_weight": jnp.clip(jax.random.uniform(streams_of[2], (D,), jnp.float32, -1.0, 1.0) * level_of(streams_of[2], (D,), ((0, 4),), -0.4, 0.0), -1.0, 1.0),
        "norm_gain": jnp.clip(1.0 + 0.1 * jax.random.normal(streams_of[3], (D,), jnp.float32), 0.5, 1.5),
        "mlp_gain": jnp.clip(1.0 + 0.1 * jax.random.normal(streams_of[4], (D,), jnp.float32), 0.5, 1.5),
        "mix_in": centred(streams_of[5], (BLOCKS, (D // BLOCKS) * (D // BLOCKS)), (D // BLOCKS) ** -0.5, 0.4375, ((0, 4),)),
        "up_weight": centred(streams_of[6], (BLOCKS, (D // BLOCKS) * (FF // BLOCKS)), (D // BLOCKS) ** -0.5, 0.4375, ((0, 4),)),
        "down_weight": centred(streams_of[7], (BLOCKS, (FF // BLOCKS) * (D // BLOCKS)), (FF // BLOCKS) ** -0.5, 0.21875, ((0, 4),)),
        "mix_out": centred(streams_of[8], (BLOCKS, (D // BLOCKS) * (D // BLOCKS)), (D // BLOCKS) ** -0.5, 0.4375, ((0, 4),)),
    }


def dft_tables(length_dft):
    position = jnp.arange(length_dft, dtype=jnp.int32)
    phase_int = position[:, None] * position[None, :] % length_dft
    radians = phase_int.astype(jnp.float32) * (2.0 * math.pi / length_dft)
    return (jnp.cos(radians).astype(jnp.bfloat16), jnp.sin(radians).astype(jnp.bfloat16))

def twiddle_tables(wide, narrow):
    outer_idx = jnp.arange(wide, dtype=jnp.int32)
    inner_idx = jnp.arange(narrow, dtype=jnp.int32)
    phase_int = outer_idx[:, None] * inner_idx[None, :] % (wide * narrow)
    radians = phase_int.astype(jnp.float32) * (2.0 * math.pi / (wide * narrow))
    return (jnp.cos(radians)[None], jnp.sin(radians)[None])

def mix_form(form, left_op, right_op):
    return jnp.einsum(form, left_op.astype(jnp.float32), right_op.astype(jnp.float32))

def forward_local(values, tables):
    cos_w, sin_w, cos_a, sin_a = tables
    rows_all, length_dft = values.shape
    wide = cos_w.shape[0]
    narrow = length_dft // wide
    grid = values.reshape(rows_all, wide, narrow)
    section_re = mix_form('rba,bk->rka', grid, cos_w)
    section_im = -mix_form('rba,bk->rka', grid, sin_w)
    twid_cos, twid_sin = twiddle_tables(wide, narrow)
    inner_re = (section_re * twid_cos + section_im * twid_sin).astype(jnp.bfloat16)
    inner_im = (section_im * twid_cos - section_re * twid_sin).astype(jnp.bfloat16)
    out_re = mix_form('rka,ad->rdk', inner_re, cos_a) + mix_form('rka,ad->rdk', inner_im, sin_a)
    out_im = mix_form('rka,ad->rdk', inner_im, cos_a) - mix_form('rka,ad->rdk', inner_re, sin_a)
    return (out_re.reshape(rows_all, length_dft), out_im.reshape(rows_all, length_dft))

def inverse_local(values_re, values_im, tables):
    cos_w, sin_w, cos_a, sin_a = tables
    rows_all, length_dft = values_re.shape
    wide = cos_w.shape[0]
    narrow = length_dft // wide
    grid_re = values_re.reshape(rows_all, narrow, wide)
    grid_im = values_im.reshape(rows_all, narrow, wide)
    back_re = mix_form('rdk,da->rka', grid_re, cos_a) - mix_form('rdk,da->rka', grid_im, sin_a)
    back_im = mix_form('rdk,da->rka', grid_im, cos_a) + mix_form('rdk,da->rka', grid_re, sin_a)
    twid_cos, twid_sin = twiddle_tables(wide, narrow)
    outer_re = (back_re * twid_cos - back_im * twid_sin).astype(jnp.bfloat16)
    outer_im = (back_im * twid_cos + back_re * twid_sin).astype(jnp.bfloat16)
    real_part = mix_form('rka,kb->rba', outer_re, cos_w) - mix_form('rka,kb->rba', outer_im, sin_w)
    return real_part.reshape(rows_all, length_dft)

def product_first(left_op, right_op):
    return jnp.dot(left_op.T, right_op, preferred_element_type=jnp.float32)

def normalize(values, gain_col):
    mean_val = lax.optimization_barrier(jnp.sum(values, axis=0, keepdims=True)) / D
    square = lax.optimization_barrier(jnp.sum(values * values, axis=0, keepdims=True)) / D
    return (values - mean_val) * lax.rsqrt(square - mean_val * mean_val + 1e-05) * gain_col[:, None]

def convolve(normed, spectrum, tables, cos_p, sin_p):
    col_width = normed.shape[0]
    share = TOK_DEV // N_SEQ
    grid = normed.reshape(col_width * N_SEQ, TOK_DEV)
    first_re, first_im = forward_local(grid, tables)
    first_re = first_re.reshape(col_width, N_SEQ, TOK_DEV)
    first_im = first_im.reshape(col_width, N_SEQ, TOK_DEV)
    frequency = jnp.arange(TOK_DEV, dtype=jnp.int32)
    devices = jnp.arange(N_SEQ, dtype=jnp.int32)
    radians = (devices[:, None] * frequency[None, :]).astype(jnp.float32) * (2.0 * math.pi / TOKENS)
    twist_cos = jnp.cos(radians)[None]
    twist_sin = jnp.sin(radians)[None]
    twisted_re = (first_re * twist_cos + first_im * twist_sin).astype(jnp.bfloat16)
    twisted_im = (first_im * twist_cos - first_re * twist_sin).astype(jnp.bfloat16)
    tw_re = twisted_re.astype(jnp.float32).reshape(col_width, N_SEQ, N_SEQ, share)
    tw_im = twisted_im.astype(jnp.float32).reshape(col_width, N_SEQ, N_SEQ, share)
    cp = cos_p.astype(jnp.float32)
    sp = sin_p.astype(jnp.float32)
    spec_re = jnp.einsum('gp,cpqr->cqgr', cp, tw_re) + jnp.einsum('gp,cpqr->cqgr', sp, tw_im)
    spec_im = jnp.einsum('gp,cpqr->cqgr', cp, tw_im) - jnp.einsum('gp,cpqr->cqgr', sp, tw_re)
    filter_re = spectrum[0].reshape(col_width, N_SEQ, N_SEQ, share)
    filter_im = spectrum[1].reshape(col_width, N_SEQ, N_SEQ, share)
    filtered_re = (filter_re * spec_re - filter_im * spec_im).astype(jnp.bfloat16).astype(jnp.float32)
    filtered_im = (filter_re * spec_im + filter_im * spec_re).astype(jnp.bfloat16).astype(jnp.float32)
    back_re = jnp.einsum('pg,cqgr->cqpr', cp, filtered_re) - jnp.einsum('pg,cqgr->cqpr', sp, filtered_im)
    back_im = jnp.einsum('pg,cqgr->cqpr', cp, filtered_im) + jnp.einsum('pg,cqgr->cqpr', sp, filtered_re)
    owned = devices[:, None] * share + jnp.arange(share, dtype=jnp.int32)[None, :]
    undo = (devices[None, :, None] * owned[:, None, :]).astype(jnp.float32) * (2.0 * math.pi / TOKENS)
    undo_cos = jnp.cos(undo)[None]
    undo_sin = jnp.sin(undo)[None]
    turned_re = (back_re * undo_cos - back_im * undo_sin).astype(jnp.bfloat16)
    turned_im = (back_im * undo_cos + back_re * undo_sin).astype(jnp.bfloat16)
    home_re = jnp.transpose(turned_re, (0, 2, 1, 3)).reshape(col_width * N_SEQ, TOK_DEV)
    home_im = jnp.transpose(turned_im, (0, 2, 1, 3)).reshape(col_width * N_SEQ, TOK_DEV)
    result = inverse_local(home_re, home_im, tables) * (1.0 / TOKENS)
    return result.reshape(col_width, TOKENS)

def reference(tokens, filter_spectrum, skip_weight, norm_gain, mlp_gain, mix_in, up_weight, down_weight, mix_out):
    inputs = tokens.astype(jnp.float32)
    normed = normalize(inputs, norm_gain).astype(jnp.bfloat16)
    cos_w, sin_w = dft_tables(RADIX)
    cos_a, sin_a = dft_tables(TOK_DEV // RADIX)
    tables = (cos_w, sin_w, cos_a, sin_a)
    cos_p, sin_p = dft_tables(N_SEQ)
    part_width = D // BLOCKS
    piece_width = part_width // BLOCKS
    hidden_width = FF // BLOCKS
    columns = []
    for block_id in range(BLOCKS):
        low_row = block_id * part_width
        columns.append(convolve(normed[low_row:low_row + part_width], filter_spectrum[:, low_row:low_row + part_width], tables, cos_p, sin_p))
    convolved = jnp.concatenate(columns, axis=0)
    residual = (inputs + convolved + skip_weight[:, None] * normed.astype(jnp.float32)).astype(jnp.bfloat16)
    second = normalize(residual.astype(jnp.float32), mlp_gain).astype(jnp.bfloat16)
    firsts = []
    for block_id in range(BLOCKS):
        low_row = block_id * part_width
        weight_block = mix_in[block_id].reshape(part_width, part_width)
        firsts.append(product_first(weight_block, second[low_row:low_row + part_width]).astype(jnp.bfloat16))
    stacked = jnp.stack(firsts, axis=0).reshape(BLOCKS, BLOCKS, piece_width, TOKENS)
    regrouped = jnp.swapaxes(stacked, 0, 1).reshape(BLOCKS, part_width, TOKENS)
    lowered = []
    for block_id in range(BLOCKS):
        up_block = up_weight[block_id].reshape(part_width, hidden_width)
        down_block = down_weight[block_id].reshape(hidden_width, part_width)
        hidden = jax.nn.gelu(product_first(up_block, regrouped[block_id]), approximate=False).astype(jnp.bfloat16)
        lowered.append(product_first(down_block, hidden).astype(jnp.bfloat16))
    lowered = jnp.stack(lowered, axis=0).reshape(BLOCKS, BLOCKS, piece_width, TOKENS)
    returned = jnp.swapaxes(lowered, 0, 1).reshape(BLOCKS, part_width, TOKENS)
    outputs = []
    for block_id in range(BLOCKS):
        outputs.append(product_first(mix_out[block_id].reshape(part_width, part_width), returned[block_id]))
    return (residual.astype(jnp.float32) + jnp.concatenate(outputs, axis=0)).astype(jnp.bfloat16)
```

```python
import functools
import math

import jax
import jax.numpy as jnp
from jax import lax
from jax.experimental import pallas as pl
from jax.experimental.pallas import tpu as pltpu
from jax.sharding import PartitionSpec as P

D = 768
CH = 192
HALF = 96
QUART = 24
TOK = 2048
NSEQ = 64
SHARE = 32
LENGTH = TOK * NSEQ
HID = 768
PIECE = 48
CHUNKS = 2
TC = TOK // CHUNKS
F32 = jnp.float32
BF16 = jnp.bfloat16
ROOT_HALF = math.sqrt(0.5)
VMEM_LIMIT = 48 * 1024 * 1024


def vm():
    return pl.BlockSpec(memory_space=pltpu.VMEM)


def sm():
    return pl.BlockSpec(memory_space=pltpu.SMEM)


def call(body, out_shape, n_smem, n_vmem, scratch=(), name=None):
    many = isinstance(out_shape, (tuple, list))
    return pl.pallas_call(
        body,
        out_shape=out_shape,
        in_specs=[sm()] * n_smem + [vm()] * n_vmem,
        out_specs=[vm() for _ in out_shape] if many else vm(),
        scratch_shapes=scratch,
        compiler_params=pltpu.CompilerParams(vmem_limit_bytes=VMEM_LIMIT),
        name=name,
    )


def shape(dims, dtype):
    return jax.ShapeDtypeStruct(dims, dtype)


def lane_group(rows):
    return lax.broadcasted_iota(jnp.int32, (rows, 128), 1)


def regroup(parts):
    rows = parts[0].shape[0]
    lane = lane_group(rows)
    low = lane < 64
    even = (lane // 32) % 2 == 0
    step = list(parts)
    for a, b in ((0, 2), (1, 3)):
        x, y = step[a], step[b]
        step[a] = jnp.where(low, x, pltpu.roll(y, 64, 1))
        step[b] = jnp.where(low, pltpu.roll(x, 64, 1), y)
    for a, b in ((0, 1), (2, 3)):
        x, y = step[a], step[b]
        step[a] = jnp.where(even, x, pltpu.roll(y, 32, 1))
        step[b] = jnp.where(even, pltpu.roll(x, 96, 1), y)
    return step


def sums_kernel(x_ref, out_ref):
    x = x_ref[...].astype(F32)
    out_ref[0:1, :] = jnp.sum(x, axis=0, keepdims=True)
    out_ref[1:2, :] = jnp.sum(x * x, axis=0, keepdims=True)


def table_kernel(alpha_ref, beta_ref, w_ref):
    def rows(b, carry):
        ac = jnp.broadcast_to(alpha_ref[0, pl.ds(b, 1), :], (SHARE, 128))
        as_ = jnp.broadcast_to(alpha_ref[1, pl.ds(b, 1), :], (SHARE, 128))
        start = pl.multiple_of(b * SHARE, SHARE)
        for u in range(8):
            bc = beta_ref[0, :, 128 * u : 128 * (u + 1)]
            bs = beta_ref[1, :, 128 * u : 128 * (u + 1)]
            w_ref[pl.ds(start, SHARE), 256 * u : 256 * u + 128] = (ac * bc - as_ * bs).astype(BF16)
            w_ref[pl.ds(start, SHARE), 256 * u + 128 : 256 * (u + 1)] = (
                -(as_ * bc + ac * bs)
            ).astype(BF16)
        return carry

    lax.fori_loop(0, NSEQ, rows, 0)


def forward_kernel(x_ref, s0, s1, s2, s3, gain_ref, w_ref, send_ref, normed_ref):
    total = s0[...] + s1[...] + s2[...] + s3[...]
    mean = total[0:1, :] / D
    square = total[1:2, :] / D
    scale = lax.rsqrt(square - mean * mean + 1e-05)
    xn = ((x_ref[...].astype(F32) - mean) * scale * gain_ref[...]).astype(BF16)
    normed_ref[...] = xn
    for u in range(8):
        y = jnp.dot(normed_ref[...], w_ref[:, 256 * u : 256 * (u + 1)], preferred_element_type=F32)
        for half in range(2):
            both = []
            for part in range(2):
                both.append(
                    regroup(
                        [
                            y[
                                half * HALF + w * QUART : half * HALF + (w + 1) * QUART,
                                128 * part : 128 * (part + 1),
                            ]
                            for w in range(4)
                        ]
                    )
                )
            for v in range(4):
                q = 4 * u + v
                dest = 63 - q if half else q
                send_ref[dest] = jnp.concatenate([both[0][v], both[1][v]], axis=0).astype(BF16)


def filter_kernel(flags, own_ref, got_ref, ca_ref, cb_ref, g_ref, g1_ref):
    high = flags[0] == 1
    first = flags[1] == 1
    row = lax.broadcasted_iota(jnp.int32, (128, 128), 0)
    lane = lax.broadcasted_iota(jnp.int32, (128, 128), 1)
    mirror = jnp.where((row + lane == 128) & (lane % SHARE != 0), 1.0, 0.0).astype(BF16)
    crow = lax.broadcasted_iota(jnp.int32, (NSEQ, 128), 0)
    clane = lax.broadcasted_iota(jnp.int32, (NSEQ, 128), 1)
    keep = jnp.where(first, 0.0, 1.0)

    def spread(target):
        return jnp.where((clane % SHARE == 0) & (crow == target + clane // SHARE), 1.0, 0.0)

    for part in range(2):
        column = (ca_ref[part].astype(F32) + cb_ref[part].astype(F32)).astype(BF16)
        for t in range(16):
            here = slice(128 * t, 128 * (t + 1))
            there = slice(128 * (15 - t), 128 * (16 - t))
            direct = jnp.where(high, got_ref[part, :, here].astype(F32), own_ref[part, :, here])
            other = jnp.where(
                high, own_ref[part, :, there], got_ref[part, :, there].astype(F32)
            ).astype(BF16)
            crossed = jnp.where(
                (clane % SHARE == 0) & (crow == 63 - 4 * t - clane // SHARE), 1.0, 0.0
            ).astype(BF16)
            mirrored = jnp.dot(other, mirror, preferred_element_type=F32) + keep * jnp.dot(
                column, crossed, preferred_element_type=F32
            )
            both = direct + mirrored if part == 0 else direct - mirrored
            out = regroup([both[w * QUART : (w + 1) * QUART] for w in range(4)])
            for v in range(4):
                g_ref[part, 4 * t + v] = out[v]

    @pl.when(first)
    def _():
        for part in range(2):
            column = (ca_ref[part].astype(F32) + cb_ref[part].astype(F32)).astype(BF16)
            for t in range(16):
                plain = spread(4 * t).astype(BF16)
                both = jnp.dot(column, plain, preferred_element_type=F32)
                out = regroup([both[w * QUART : (w + 1) * QUART] for w in range(4)])
                for v in range(4):
                    g1_ref[part, 4 * t + v] = out[v]


def turn_i(re, im, s):
    return (-im, re) if s > 0 else (im, -re)


def dft4(xr, xi, s):
    ar, ai = xr[0] + xr[2], xi[0] + xi[2]
    br, bi = xr[0] - xr[2], xi[0] - xi[2]
    cr, ci = xr[1] + xr[3], xi[1] + xi[3]
    dr, di = turn_i(xr[1] - xr[3], xi[1] - xi[3], s)
    return [ar + cr, br + dr, ar - cr, br - dr], [ai + ci, bi + di, ai - ci, bi - di]


def dft8(xr, xi, s):
    er, ei = dft4(xr[0::2], xi[0::2], s)
    dr, di = dft4(xr[1::2], xi[1::2], s)
    c = ROOT_HALF
    if s > 0:
        dr1, di1 = c * (dr[1] - di[1]), c * (di[1] + dr[1])
        dr3, di3 = -c * (dr[3] + di[3]), c * (dr[3] - di[3])
    else:
        dr1, di1 = c * (dr[1] + di[1]), c * (di[1] - dr[1])
        dr3, di3 = c * (di[3] - dr[3]), -c * (di[3] + dr[3])
    dr2, di2 = turn_i(dr[2], di[2], s)
    qr = [dr[0], dr1, dr2, dr3]
    qi = [di[0], di1, di2, di3]
    return (
        [er[k] + qr[k] for k in range(4)] + [er[k] - qr[k] for k in range(4)],
        [ei[k] + qi[k] for k in range(4)] + [ei[k] - qi[k] for k in range(4)],
    )


def twiddle(re, im, index, s):
    index %= 64
    if index == 0:
        return re, im
    c = math.cos(2.0 * math.pi * index / 64.0)
    d = s * math.sin(2.0 * math.pi * index / 64.0)
    return re * c - im * d, im * c + re * d


def across(load, store, gains, a_ref, b_ref):
    for p0 in range(8):
        xr, xi = zip(*[load(p0 + 8 * p1) for p1 in range(8)])
        yr, yi = dft8(list(xr), list(xi), -1)
        for g1 in range(8):
            a_ref[0, g1 * 8 + p0], a_ref[1, g1 * 8 + p0] = twiddle(yr[g1], yi[g1], p0 * g1, -1)
    for g1 in range(8):
        yr, yi = dft8(
            [a_ref[0, g1 * 8 + p0] for p0 in range(8)],
            [a_ref[1, g1 * 8 + p0] for p0 in range(8)],
            -1,
        )
        for g2 in range(8):
            hr, hi = gains(g1 + 8 * g2)
            yr[g2], yi[g2] = hr * yr[g2] - hi * yi[g2], hr * yi[g2] + hi * yr[g2]
        zr, zi = dft8(yr, yi, 1)
        for p0 in range(8):
            b_ref[0, p0 * 8 + g1], b_ref[1, p0 * 8 + g1] = twiddle(zr[p0], zi[p0], g1 * p0, 1)
    for p0 in range(8):
        zr, zi = dft8(
            [b_ref[0, p0 * 8 + g1] for g1 in range(8)],
            [b_ref[1, p0 * 8 + g1] for g1 in range(8)],
            1,
        )
        for p1 in range(8):
            store(p0 + 8 * p1, zr[p1], zi[p1])


def middle_kernel(flags, got_ref, g_ref, g1_ref, out_ref, xs, a_ref, b_ref, t1):
    first = flags[1] == 1
    special = (lane_group(8) % SHARE == 0) & first

    def widen(p, carry):
        xs[p] = got_ref[p].astype(F32)
        return carry

    lax.fori_loop(0, NSEQ, widen, 0)

    def half_turn(p):
        return math.cos(2.0 * math.pi * p / 128.0), math.sin(2.0 * math.pi * p / 128.0)

    @pl.when(first)
    def _():
        def alone(i, carry):
            top = pl.ds(pl.multiple_of(i * 8, 8), 8)
            bottom = pl.ds(pl.multiple_of(i * 8 + QUART, 8), 8)

            def load(p):
                c, s = half_turn(p)
                im = jnp.where(special, xs[p, bottom, :], 0.0)
                return im * c, im * (-s)

            def store(p, re, im):
                c, s = half_turn(p)
                t1[p, top, :] = re * c - im * s

            across(load, store, lambda g: (g1_ref[0, g, top, :], g1_ref[1, g, top, :]), a_ref, b_ref)
            return carry

        lax.fori_loop(0, 3, alone, 0)

    def every(i, carry):
        top = pl.ds(pl.multiple_of(i * 8, 8), 8)
        bottom = pl.ds(pl.multiple_of(i * 8 + QUART, 8), 8)

        def load(p):
            return xs[p, top, :], jnp.where(special, 0.0, xs[p, bottom, :])

        def store(p, re, im):
            xs[p, top, :] = re
            xs[p, bottom, :] = jnp.where(special, t1[p, top, :], im)

        across(load, store, lambda g: (g_ref[0, g, top, :], g_ref[1, g, top, :]), a_ref, b_ref)
        return carry

    lax.fori_loop(0, 3, every, 0)

    def narrow(p, carry):
        out_ref[p] = xs[p].astype(BF16)
        return carry

    lax.fori_loop(0, NSEQ, narrow, 0)


def back_kernel(
    flags, got_ref, w_ref, x_ref, normed_ref, skip_ref, gain_ref, gain_row, mix_ref, mix_t_ref,
    res_ref, st_ref, u0, u1, u2, u3, tm,
):
    for half in range(2):
        for u in range(8):
            parts = []
            for v in range(4):
                q = 4 * u + v
                parts.append(got_ref[63 - q if half else q].astype(F32))
            out = regroup(parts)
            for w in range(4):
                low = half * HALF + w * QUART
                tm[low : low + QUART, 256 * u : 256 * u + 128] = out[w][:QUART]
                tm[low : low + QUART, 256 * u + 128 : 256 * (u + 1)] = out[w][QUART:]
    values = tm[...].astype(BF16)
    outs = (u0, u1, u2, u3)
    me = flags[2]
    st_ref[2:3, :] = jnp.zeros((1, TOK), F32)
    st_ref[3:4, :] = jnp.zeros((1, TOK), F32)
    st_ref[2:3, 0:CH] = jnp.dot(
        gain_row[...], mix_ref[...].astype(F32), preferred_element_type=F32,
        precision=lax.Precision.HIGHEST,
    )
    for n in range(8):
        cols = slice(256 * n, 256 * (n + 1))
        conv = lax.dot_general(
            values, w_ref[cols, :], (((1,), (1,)), ((), ())), preferred_element_type=F32
        )
        res = (
            x_ref[:, cols].astype(F32)
            + conv * (1.0 / LENGTH)
            + skip_ref[...] * normed_ref[:, cols].astype(F32)
        ).astype(BF16)
        res_ref[:, cols] = res
        r = res.astype(F32)
        mean = jnp.sum(r, axis=0, keepdims=True) * (1.0 / CH)
        centred = r - mean
        st_ref[0:1, cols] = mean
        st_ref[1:2, cols] = jnp.sum(centred * centred, axis=0, keepdims=True)
        z = (centred * gain_ref[...]).astype(BF16)
        tm[:, cols] = jnp.dot(mix_t_ref[...], z, preferred_element_type=F32)
    for k in range(4):
        rows = pl.ds(pl.multiple_of((me ^ k) * PIECE, PIECE), PIECE)
        outs[k][...] = tm[rows, :].astype(BF16)


def mlp_kernel(
    flags, p0, p1, p2, p3, s0, s1, s2, s3, up_t, down_t, o0, o1, o2, o3, f_ref, low_ref, *, chunk
):
    me = flags[2]
    here = slice(chunk * TC, (chunk + 1) * TC)
    stats = [s[...] for s in (s0, s1, s2, s3)]
    means = [s[0:1, here] for s in stats]
    mean = (means[0] + means[1] + means[2] + means[3]) * 0.25
    spread = sum(s[1:2, here] for s in stats) + CH * sum((m - mean) * (m - mean) for m in means)
    scale = lax.rsqrt(spread * (1.0 / D) + 1e-05)
    row = lax.broadcasted_iota(jnp.int32, (PIECE, CH), 0)
    lane = lax.broadcasted_iota(jnp.int32, (PIECE, CH), 1)
    pick = lane == row + me * PIECE
    for k, p in enumerate((p0, p1, p2, p3)):
        weight = jnp.sum(jnp.where(pick, stats[k][2:3, 0:CH], 0.0), axis=1, keepdims=True)
        value = scale * (p[...].astype(F32) - (mean - means[k]) * weight)
        f_ref[pl.ds(pl.multiple_of((me ^ k) * PIECE, PIECE), PIECE), :] = value
    for n in range(TC // 256):
        cols = slice(256 * n, 256 * (n + 1))
        f = f_ref[:, cols].astype(BF16)
        total = None
        for h in range(3):
            rows = slice(256 * h, 256 * (h + 1))
            wide = jnp.dot(up_t[rows, :], f, preferred_element_type=F32)
            act = (0.5 * wide * (1.0 + lax.erf(wide * ROOT_HALF))).astype(BF16)
            part = jnp.dot(down_t[:, rows], act, preferred_element_type=F32)
            total = part if total is None else total + part
        low_ref[:, cols] = total
    for k, o in enumerate((o0, o1, o2, o3)):
        o[...] = low_ref[pl.ds(pl.multiple_of((me ^ k) * PIECE, PIECE), PIECE), :].astype(BF16)


def final_kernel(flags, *refs):
    pieces = (refs[0:4], refs[4:8])
    res_ref, mix_t_ref, out_ref, f_ref = refs[8:]
    me = flags[2]
    for c in range(CHUNKS):
        here = slice(c * TC, (c + 1) * TC)
        for k in range(4):
            rows = pl.ds(pl.multiple_of((me ^ k) * PIECE, PIECE), PIECE)
            f_ref[rows, here] = pieces[c][k][...].astype(F32)
        for n in range(TC // 256):
            cols = slice(c * TC + 256 * n, c * TC + 256 * (n + 1))
            add = jnp.dot(mix_t_ref[...], f_ref[:, cols].astype(BF16), preferred_element_type=F32)
            out_ref[:, cols] = (res_ref[:, cols].astype(F32) + add).astype(BF16)


def swap(x, k):
    return lax.ppermute(x, "chan", [(i, i ^ k) for i in range(4)])


def shards(
    tokens, filter_spectrum, skip_weight, norm_gain, mlp_gain, mix_in, up_weight, down_weight, mix_out
):
    place = lax.axis_index("seq")
    lane_of = lax.axis_index("chan")
    high = place >= 32
    first = (place == 0) | (place == 63)
    flags = jnp.stack([high, first, lane_of, place]).astype(jnp.int32)
    mine = jnp.where(high, HALF, 0)
    theirs = jnp.where(high, 0, HALF)
    give = lax.dynamic_slice_in_dim(filter_spectrum, theirs, HALF, 1).astype(BF16)
    got = lax.ppermute(give, "seq", [(i, 63 - i) for i in range(64)])
    sums = call(sums_kernel, shape((2, TOK), F32), 0, 1, name="sums")(tokens)
    others = [swap(sums, k) for k in (1, 2, 3)]
    own = lax.dynamic_slice_in_dim(filter_spectrum, mine, HALF, 1)
    pick_row = jnp.arange(TOK, dtype=jnp.int32)[:, None]
    pick_col = jnp.arange(NSEQ, dtype=jnp.int32)[None, :]
    pick = (pick_row == SHARE * pick_col).astype(BF16)
    column = jnp.einsum(
        "pcj,jg->pcg", filter_spectrum.astype(BF16), pick, preferred_element_type=F32
    ).astype(BF16)
    ca = lax.ppermute(column[:, :HALF], "seq", [(32, 0)] + [(64 - i, i) for i in range(1, 32)])
    cb = lax.ppermute(column[:, HALF:], "seq", [(32, 63)] + [(i + 1, i) for i in range(32, 63)])
    freq = jnp.arange(TOK // 2, dtype=jnp.int32)
    step = jnp.arange(SHARE, dtype=jnp.int32)
    angle = (freq[None, :] * (64 * step[:, None] + place) % LENGTH).astype(F32) * (
        2.0 * math.pi / LENGTH
    )
    parity = 1.0 - 2.0 * (step % 2).astype(F32)
    beta = jnp.stack(
        [jnp.cos(angle), jnp.where(freq[None, :] == 0, -parity[:, None], jnp.sin(angle))]
    )
    turn = (
        (jnp.arange(NSEQ, dtype=jnp.int32)[:, None] * (jnp.arange(128, dtype=jnp.int32)[None, :])) % 64
    ).astype(F32) * (2.0 * math.pi / 64)
    alpha = jnp.stack([jnp.cos(turn), jnp.sin(turn)])
    table = call(table_kernel, shape((TOK, TOK), BF16), 0, 2, name="table")(alpha, beta)
    send, normed = call(
        forward_kernel,
        (shape((NSEQ, 2 * QUART, 128), BF16), shape((CH, TOK), BF16)),
        0,
        7,
        name="forward",
    )(tokens, sums, *others, norm_gain[:, None], table)
    moved = lax.all_to_all(send, "seq", split_axis=0, concat_axis=0, tiled=True)
    gains, gains_first = call(
        filter_kernel,
        (shape((2, NSEQ, QUART, 128), F32), shape((2, NSEQ, QUART, 128), F32)),
        1,
        4,
        name="gains",
    )(flags, own, got, ca, cb)
    mix_in_full = mix_in.reshape(CH, CH)
    mix_in_t = mix_in_full.T
    mix_out_t = mix_out.reshape(CH, CH).T
    up_t = up_weight.reshape(CH, HID).T
    down_t = down_weight.reshape(HID, CH).T
    moved, gains, gains_first, mix_in_full, mix_in_t, mix_out_t, up_t, down_t = (
        lax.optimization_barrier(
            (moved, gains, gains_first, mix_in_full, mix_in_t, mix_out_t, up_t, down_t)
        )
    )
    back = call(
        middle_kernel,
        shape((NSEQ, 2 * QUART, 128), BF16),
        1,
        3,
        scratch=[
            pltpu.VMEM((NSEQ, 2 * QUART, 128), F32),
            pltpu.VMEM((2, NSEQ, 8, 128), F32),
            pltpu.VMEM((2, NSEQ, 8, 128), F32),
            pltpu.VMEM((NSEQ, QUART, 128), F32),
        ],
        name="middle",
    )(flags, moved, gains, gains_first)
    home = lax.all_to_all(back, "seq", split_axis=0, concat_axis=0, tiled=True)
    residual, stats, *firsts = call(
        back_kernel,
        (shape((CH, TOK), BF16), shape((4, TOK), F32)) + (shape((PIECE, TOK), BF16),) * 4,
        1,
        9,
        scratch=[pltpu.VMEM((CH, TOK), F32)],
        name="back",
    )(
        flags, home, table, tokens, normed, skip_weight[:, None], mlp_gain[:, None],
        mlp_gain[None, :], mix_in_full, mix_in_t,
    )
    all_stats = [stats] + [swap(stats, k) for k in (1, 2, 3)]
    arrived = []
    for c in range(CHUNKS):
        pieces = [f[:, c * TC : (c + 1) * TC] for f in firsts]
        arrived.append([pieces[0]] + [swap(pieces[k], k) for k in (1, 2, 3)])
    returned = []
    for c in range(CHUNKS):
        lows = call(
            functools.partial(mlp_kernel, chunk=c),
            (shape((PIECE, TC), BF16),) * 4,
            1,
            10,
            scratch=[pltpu.VMEM((CH, TC), F32), pltpu.VMEM((CH, TC), F32)],
            name="mlp",
        )(flags, *arrived[c], *all_stats, up_t, down_t)
        returned.append([lows[0]] + [swap(lows[k], k) for k in (1, 2, 3)])
    return call(
        final_kernel,
        shape((CH, TOK), BF16),
        1,
        10,
        scratch=[pltpu.VMEM((CH, TOK), F32)],
        name="final",
    )(flags, *returned[0], *returned[1], residual, mix_out_t)


def solution(mesh):
    in_specs = (
        P("chan", "seq"),
        P(None, "chan", "seq"),
        P("chan"),
        P("chan"),
        P("chan"),
        P("chan", None),
        P("chan", None),
        P("chan", None),
        P("chan", None),
    )
    out_specs = P("chan", "seq")
    return jax.shard_map(shards, mesh=mesh, in_specs=in_specs, out_specs=out_specs, check_vma=False)
```

```python
import math

import jax
import jax.numpy as jnp
from jax import lax
from jax.experimental import pallas as pl
from jax.experimental.pallas import tpu as pltpu
from jax.sharding import PartitionSpec as P


D = 768
CH = 192
HALF = 96
QUART = 24
TOK = 2048
NSEQ = 64
SHARE = 32
LENGTH = TOK * NSEQ
HID = 768
PIECE = 48
CHUNKS = 2
TC = TOK // CHUNKS
F32 = jnp.float32
BF16 = jnp.bfloat16
ROOT_HALF = math.sqrt(0.5)
MIB = 1024 * 1024
ROWS = 56


def vm():
    return pl.BlockSpec(memory_space=pltpu.VMEM)


def sm():
    return pl.BlockSpec(memory_space=pltpu.SMEM)


def hb():
    return pl.BlockSpec(memory_space=pltpu.HBM)


def call(body, out_shape, kinds, scratch=(), mib=14, outs=None):
    spec = {"s": sm, "v": vm, "h": hb}
    many = isinstance(out_shape, (tuple, list))
    outs = outs or "v" * (len(out_shape) if many else 1)
    return pl.pallas_call(
        body,
        out_shape=out_shape,
        in_specs=[spec[k]() for k in kinds],
        out_specs=[spec[k]() for k in outs] if many else spec[outs](),
        scratch_shapes=scratch,
        compiler_params=pltpu.CompilerParams(vmem_limit_bytes=mib * MIB),
    )


def in_hbm(x):
    return pltpu.with_memory_space_constraint(x, pltpu.HBM)


def shape(dims, dtype):
    return jax.ShapeDtypeStruct(dims, dtype)


def lane_group(rows):
    return lax.broadcasted_iota(jnp.int32, (rows, 128), 1)


def regroup(parts):
    rows = parts[0].shape[0]
    lane = lane_group(rows)
    low = lane < 64
    even = (lane // 32) % 2 == 0
    step = list(parts)
    for a, b in ((0, 2), (1, 3)):
        x, y = step[a], step[b]
        step[a] = jnp.where(low, x, pltpu.roll(y, 64, 1))
        step[b] = jnp.where(low, pltpu.roll(x, 64, 1), y)
    for a, b in ((0, 1), (2, 3)):
        x, y = step[a], step[b]
        step[a] = jnp.where(even, x, pltpu.roll(y, 32, 1))
        step[b] = jnp.where(even, pltpu.roll(x, 96, 1), y)
    return step


def column_of(row_ref):
    n = row_ref.shape[1]
    eye = lax.broadcasted_iota(jnp.int32, (n, n), 0) == lax.broadcasted_iota(jnp.int32, (n, n), 1)
    return jnp.sum(jnp.where(eye, row_ref[...], 0.0), axis=1, keepdims=True)


def sums_kernel(x_ref, out_ref):
    x = x_ref[...].astype(F32)
    out_ref[0:1, :] = jnp.sum(x, axis=0, keepdims=True)
    out_ref[1:2, :] = jnp.sum(x * x, axis=0, keepdims=True)


def table_kernel(flags, alpha_ref, beta_ref, filter_ref, w_ref, give_ref, held, sem):
    theirs = pl.multiple_of((1 - flags[0]) * HALF, HALF)
    fetch = pltpu.make_async_copy(filter_ref.at[:, pl.ds(theirs, HALF), :], held, sem)
    fetch.start()

    def rows(b, carry):
        ac = jnp.broadcast_to(alpha_ref[0, pl.ds(b, 1), :], (SHARE, 128))
        as_ = jnp.broadcast_to(alpha_ref[1, pl.ds(b, 1), :], (SHARE, 128))
        start = pl.multiple_of(b * SHARE, SHARE)
        for u in range(8):
            bc = beta_ref[0, :, 128 * u : 128 * (u + 1)]
            bs = beta_ref[1, :, 128 * u : 128 * (u + 1)]
            w_ref[pl.ds(start, SHARE), 256 * u : 256 * u + 128] = (ac * bc - as_ * bs).astype(BF16)
            w_ref[pl.ds(start, SHARE), 256 * u + 128 : 256 * (u + 1)] = (
                -(as_ * bc + ac * bs)
            ).astype(BF16)
        return carry

    lax.fori_loop(0, NSEQ, rows, 0)
    fetch.wait()
    give_ref[...] = held[...].astype(BF16)


def forward_kernel(x_ref, s0, s1, s2, s3, gain_ref, w_ref, send_ref, normed_ref):
    total = s0[...] + s1[...] + s2[...] + s3[...]
    mean = total[0:1, :] / D
    square = total[1:2, :] / D
    scale = lax.rsqrt(square - mean * mean + 1e-05)
    xn = ((x_ref[...].astype(F32) - mean) * scale * column_of(gain_ref)).astype(BF16)
    normed_ref[...] = xn
    for u in range(8):
        y = jnp.dot(normed_ref[...], w_ref[:, 256 * u : 256 * (u + 1)], preferred_element_type=F32)
        for half in range(2):
            both = []
            for part in range(2):
                both.append(
                    regroup(
                        [
                            y[
                                half * HALF + w * QUART : half * HALF + (w + 1) * QUART,
                                128 * part : 128 * (part + 1),
                            ]
                            for w in range(4)
                        ]
                    )
                )
            for v in range(4):
                q = 4 * u + v
                dest = 63 - q if half else q
                send_ref[dest] = jnp.concatenate([both[0][v], both[1][v]], axis=0).astype(BF16)


def filter_kernel(
    flags, own_ref, got_ref, ca_ref, cb_ref, g_out, g1_out, g_ref, g1_ref, sems
):
    high = flags[0] == 1
    first = flags[1] == 1
    row = lax.broadcasted_iota(jnp.int32, (128, 128), 0)
    lane = lax.broadcasted_iota(jnp.int32, (128, 128), 1)
    mirror = jnp.where((row + lane == 128) & (lane % SHARE != 0), 1.0, 0.0).astype(BF16)
    crow = lax.broadcasted_iota(jnp.int32, (NSEQ, 128), 0)
    clane = lax.broadcasted_iota(jnp.int32, (NSEQ, 128), 1)
    keep = jnp.where(first, 0.0, 1.0)

    def spread(target):
        return jnp.where((clane % SHARE == 0) & (crow == target + clane // SHARE), 1.0, 0.0)

    for part in range(2):
        column = (ca_ref[part].astype(F32) + cb_ref[part].astype(F32)).astype(BF16)
        for t in range(16):
            here = slice(128 * t, 128 * (t + 1))
            there = slice(128 * (15 - t), 128 * (16 - t))
            direct = jnp.where(high, got_ref[part, :, here].astype(F32), own_ref[part, :, here])
            other = jnp.where(
                high, own_ref[part, :, there], got_ref[part, :, there].astype(F32)
            ).astype(BF16)
            crossed = jnp.where(
                (clane % SHARE == 0) & (crow == 63 - 4 * t - clane // SHARE), 1.0, 0.0
            ).astype(BF16)
            mirrored = jnp.dot(other, mirror, preferred_element_type=F32) + keep * jnp.dot(
                column, crossed, preferred_element_type=F32
            )
            both = direct + mirrored if part == 0 else direct - mirrored
            out = regroup([both[w * QUART : (w + 1) * QUART] for w in range(4)])
            for v in range(4):
                g_ref[part, 4 * t + v] = out[v]
        pltpu.make_async_copy(g_ref.at[part], g_out.at[part], sems.at[part]).start()

    @pl.when(first)
    def _():
        for part in range(2):
            column = (ca_ref[part].astype(F32) + cb_ref[part].astype(F32)).astype(BF16)
            for t in range(16):
                plain = spread(4 * t).astype(BF16)
                both = jnp.dot(column, plain, preferred_element_type=F32)
                out = regroup([both[w * QUART : (w + 1) * QUART] for w in range(4)])
                for v in range(4):
                    g1_ref[part, 4 * t + v] = out[v]
        last = pltpu.make_async_copy(g1_ref, g1_out, sems.at[2])
        last.start()
        last.wait()

    for part in range(2):
        pltpu.make_async_copy(g_ref.at[part], g_out.at[part], sems.at[part]).wait()


def turn_i(re, im, s):
    return (-im, re) if s > 0 else (im, -re)


def dft4(xr, xi, s):
    ar, ai = xr[0] + xr[2], xi[0] + xi[2]
    br, bi = xr[0] - xr[2], xi[0] - xi[2]
    cr, ci = xr[1] + xr[3], xi[1] + xi[3]
    dr, di = turn_i(xr[1] - xr[3], xi[1] - xi[3], s)
    return [ar + cr, br + dr, ar - cr, br - dr], [ai + ci, bi + di, ai - ci, bi - di]


def dft8(xr, xi, s):
    er, ei = dft4(xr[0::2], xi[0::2], s)
    dr, di = dft4(xr[1::2], xi[1::2], s)
    c = ROOT_HALF
    if s > 0:
        dr1, di1 = c * (dr[1] - di[1]), c * (di[1] + dr[1])
        dr3, di3 = -c * (dr[3] + di[3]), c * (dr[3] - di[3])
    else:
        dr1, di1 = c * (dr[1] + di[1]), c * (di[1] - dr[1])
        dr3, di3 = c * (di[3] - dr[3]), -c * (di[3] + dr[3])
    dr2, di2 = turn_i(dr[2], di[2], s)
    qr = [dr[0], dr1, dr2, dr3]
    qi = [di[0], di1, di2, di3]
    return (
        [er[k] + qr[k] for k in range(4)] + [er[k] - qr[k] for k in range(4)],
        [ei[k] + qi[k] for k in range(4)] + [ei[k] - qi[k] for k in range(4)],
    )


def twiddle(re, im, index, s):
    index %= 64
    if index == 0:
        return re, im
    c = math.cos(2.0 * math.pi * index / 64.0)
    d = s * math.sin(2.0 * math.pi * index / 64.0)
    return re * c - im * d, im * c + re * d


def across(load, store, gains, a_ref, b_ref):
    for p0 in range(8):
        xr, xi = zip(*[load(p0 + 8 * p1) for p1 in range(8)])
        yr, yi = dft8(list(xr), list(xi), -1)
        for g1 in range(8):
            a_ref[0, g1 * 8 + p0], a_ref[1, g1 * 8 + p0] = twiddle(yr[g1], yi[g1], p0 * g1, -1)
    for g1 in range(8):
        yr, yi = dft8(
            [a_ref[0, g1 * 8 + p0] for p0 in range(8)],
            [a_ref[1, g1 * 8 + p0] for p0 in range(8)],
            -1,
        )
        for g2 in range(8):
            hr, hi = gains(g1 + 8 * g2)
            yr[g2], yi[g2] = hr * yr[g2] - hi * yi[g2], hr * yi[g2] + hi * yr[g2]
        zr, zi = dft8(yr, yi, 1)
        for p0 in range(8):
            b_ref[0, p0 * 8 + g1], b_ref[1, p0 * 8 + g1] = twiddle(zr[p0], zi[p0], g1 * p0, 1)
    for p0 in range(8):
        zr, zi = dft8(
            [b_ref[0, p0 * 8 + g1] for g1 in range(8)],
            [b_ref[1, p0 * 8 + g1] for g1 in range(8)],
            1,
        )
        for p1 in range(8):
            store(p0 + 8 * p1, zr[p1], zi[p1])


def middle_kernel(
    flags, got_ref, g_in, g1_in, out_ref, xs, a_ref, b_ref, t1, g_ref, g1_ref, sems
):
    first = flags[1] == 1
    gains = pltpu.make_async_copy(g_in, g_ref, sems.at[0])
    gains.start()
    special = (lane_group(8) % SHARE == 0) & first

    def widen(p, carry):
        xs[p] = got_ref[p].astype(F32)
        return carry

    lax.fori_loop(0, NSEQ, widen, 0)

    def half_turn(p):
        return math.cos(2.0 * math.pi * p / 128.0), math.sin(2.0 * math.pi * p / 128.0)

    @pl.when(first)
    def _():
        fetch = pltpu.make_async_copy(g1_in, g1_ref, sems.at[1])
        fetch.start()
        fetch.wait()

        def alone(i, carry):
            top = pl.ds(pl.multiple_of(i * 8, 8), 8)
            bottom = pl.ds(pl.multiple_of(i * 8 + QUART, 8), 8)

            def load(p):
                c, s = half_turn(p)
                im = jnp.where(special, xs[p, bottom, :], 0.0)
                return im * c, im * (-s)

            def store(p, re, im):
                c, s = half_turn(p)
                t1[p, top, :] = re * c - im * s

            across(load, store, lambda g: (g1_ref[0, g, top, :], g1_ref[1, g, top, :]), a_ref, b_ref)
            return carry

        lax.fori_loop(0, 3, alone, 0)

    gains.wait()

    def every(i, carry):
        top = pl.ds(pl.multiple_of(i * 8, 8), 8)
        bottom = pl.ds(pl.multiple_of(i * 8 + QUART, 8), 8)

        def load(p):
            return xs[p, top, :], jnp.where(special, 0.0, xs[p, bottom, :])

        def store(p, re, im):
            xs[p, top, :] = re
            xs[p, bottom, :] = jnp.where(special, t1[p, top, :], im)

        across(load, store, lambda g: (g_ref[0, g, top, :], g_ref[1, g, top, :]), a_ref, b_ref)
        return carry

    lax.fori_loop(0, 3, every, 0)

    def narrow(p, carry):
        out_ref[p] = xs[p].astype(BF16)
        return carry

    lax.fori_loop(0, NSEQ, narrow, 0)


def in_three(x):
    a = x.astype(BF16)
    rest = x - a.astype(F32)
    b = rest.astype(BF16)
    return [a, b, (rest - b.astype(F32)).astype(BF16)]


def tokens_back(
    flags, values, w_ref, x_ref, normed_ref, skip_row, gain_row, mix_ref, mix_t_ref, res_ref, outs, tm, st,
    fetches,
    chunk,
):
    me = flags[2]
    skip = column_of(skip_row)
    gain = column_of(gain_row)
    st[...] = jnp.zeros((8, TC), F32)
    weight = jnp.dot(
        gain_row[...], mix_ref[...].astype(F32), preferred_element_type=F32,
        precision=lax.Precision.HIGHEST,
    )
    for k, part in enumerate(in_three(weight)[:2]):
        st[5 + k : 6 + k, 0:CH] = part.astype(F32)
    for n in range(TC // 256):
        here = slice(256 * n, 256 * (n + 1))
        cols = slice(chunk * TC + 256 * n, chunk * TC + 256 * (n + 1))
        fetches[n].wait()
        conv = lax.dot_general(
            values, w_ref[here, :], (((1,), (1,)), ((), ())), preferred_element_type=F32
        )
        res = (
            x_ref[:, cols].astype(F32)
            + conv * (1.0 / LENGTH)
            + skip * normed_ref[:, cols].astype(F32)
        ).astype(BF16)
        res_ref[:, here] = res
        r = res.astype(F32)
        mean = jnp.sum(r, axis=0, keepdims=True) * (1.0 / CH)
        centred = r - mean
        for k, part in enumerate(in_three(mean)):
            st[k : k + 1, here] = part.astype(F32)
        for k, part in enumerate(in_three(jnp.sum(centred * centred, axis=0, keepdims=True))[:2]):
            st[3 + k : 4 + k, here] = part.astype(F32)
        z = (centred * gain).astype(BF16)
        tm[:, here] = jnp.dot(mix_t_ref[...], z, preferred_element_type=F32)
    for k in range(4):
        rows = pl.ds(pl.multiple_of((me ^ k) * PIECE, PIECE), PIECE)
        outs[k][...] = jnp.concatenate([tm[rows, :], st[...]], axis=0).astype(BF16)


def fetch_table(w_hbm, w_ref, sems, chunk):
    fetches = []
    for n in range(TC // 256):
        here = slice(256 * n, 256 * (n + 1))
        there = slice(chunk * TC + 256 * n, chunk * TC + 256 * (n + 1))
        fetches.append(pltpu.make_async_copy(w_hbm.at[there, :], w_ref.at[here, :], sems.at[n]))
        fetches[-1].start()
    return fetches


def back_first_kernel(
    flags, got_ref, w_hbm, x_ref, normed_ref, skip_row, gain_row, mix_ref, mix_t_ref,
    values_ref, res_ref, u0, u1, u2, u3, tall, tm, st, w_ref, sems,
):
    fetches = fetch_table(w_hbm, w_ref, sems, 0)
    for half in range(2):
        for u in range(8):
            parts = []
            for v in range(4):
                q = 4 * u + v
                parts.append(got_ref[63 - q if half else q].astype(F32))
            out = regroup(parts)
            for w in range(4):
                low = half * HALF + w * QUART
                tall[low : low + QUART, 256 * u : 256 * u + 128] = out[w][:QUART]
                tall[low : low + QUART, 256 * u + 128 : 256 * (u + 1)] = out[w][QUART:]
    values = tall[...].astype(BF16)
    values_ref[...] = values
    tokens_back(
        flags, values_ref[...], w_ref, x_ref, normed_ref, skip_row, gain_row, mix_ref, mix_t_ref, res_ref,
        (u0, u1, u2, u3), tm, st, fetches, 0,
    )


def back_second_kernel(
    flags, values_ref, w_hbm, x_ref, normed_ref, skip_row, gain_row, mix_ref, mix_t_ref,
    res_ref, u0, u1, u2, u3, tm, st, w_ref, sems,
):
    fetches = fetch_table(w_hbm, w_ref, sems, 1)
    tokens_back(
        flags, values_ref[...], w_ref, x_ref, normed_ref, skip_row, gain_row, mix_ref, mix_t_ref, res_ref,
        (u0, u1, u2, u3), tm, st, fetches, 1,
    )


def mlp_kernel(flags, p0, p1, p2, p3, up_t, down_t, o0, o1, o2, o3, f_ref, low_ref):
    me = flags[2]
    values = [p[...].astype(F32) for p in (p0, p1, p2, p3)]
    tails = [x[PIECE:ROWS] for x in values]
    means = [t[0:1] + t[1:2] + t[2:3] for t in tails]
    mean = (means[0] + means[1] + means[2] + means[3]) * 0.25
    spread = sum(t[3:4] + t[4:5] for t in tails) + CH * sum((m - mean) * (m - mean) for m in means)
    scale = lax.rsqrt(spread * (1.0 / D) + 1e-05)
    row = lax.broadcasted_iota(jnp.int32, (PIECE, CH), 0)
    lane = lax.broadcasted_iota(jnp.int32, (PIECE, CH), 1)
    pick = lane == row + me * PIECE
    for k in range(4):
        line = tails[k][5:6, 0:CH] + tails[k][6:7, 0:CH]
        weight = jnp.sum(jnp.where(pick, line, 0.0), axis=1, keepdims=True)
        f_ref[pl.ds(pl.multiple_of((me ^ k) * PIECE, PIECE), PIECE), :] = scale * (
            values[k][:PIECE] - (mean - means[k]) * weight
        )
    for n in range(TC // 256):
        cols = slice(256 * n, 256 * (n + 1))
        f = f_ref[:, cols].astype(BF16)
        total = None
        for h in range(3):
            rows = slice(256 * h, 256 * (h + 1))
            wide = jnp.dot(up_t[rows, :], f, preferred_element_type=F32)
            act = (0.5 * wide * (1.0 + lax.erf(wide * ROOT_HALF))).astype(BF16)
            part = jnp.dot(down_t[:, rows], act, preferred_element_type=F32)
            total = part if total is None else total + part
        low_ref[:, cols] = total
    for k, o in enumerate((o0, o1, o2, o3)):
        o[...] = low_ref[pl.ds(pl.multiple_of((me ^ k) * PIECE, PIECE), PIECE), :].astype(BF16)


def weights_kernel(
    mix_in_ref, up_ref, down_ref, mix_out_ref, in_ref, in_t, up_t, down_t, out_t, square, wide, tall
):
    def unroll(src, dst, rows, cols):
        def step(i, carry):
            for k in range(8):
                row = i * 8 + k
                start = pl.multiple_of(row * cols, 128)
                dst[pl.ds(row, 1), :] = src[:, pl.ds(start, cols)].astype(F32)
            return carry

        lax.fori_loop(0, rows // 8, step, 0)

    unroll(up_ref, wide, CH, HID)
    up_t[...] = wide[...].T.astype(BF16)
    for src, dst in ((mix_in_ref, in_t), (mix_out_ref, out_t)):
        paired(src, square, CH)
        if dst is in_t:
            in_ref[...] = square[...].astype(BF16)
        dst[...] = square[...].T.astype(BF16)
    paired(down_ref, tall, HID)
    down_t[...] = tall[...].T.astype(BF16)


def paired(src, dst, rows):
    def step(i, carry):
        for k in range(4):
            row = i * 8 + 2 * k
            start = pl.multiple_of(row * CH, 128)
            both = src[:, pl.ds(start, 2 * CH)].astype(F32)
            dst[pl.ds(row, 1), :] = both[:, :CH]
            dst[pl.ds(row + 1, 1), :] = both[:, CH:]
        return carry

    lax.fori_loop(0, rows // 8, step, 0)


def tokens_out(flags, pieces, res_ref, mix_t_ref, f_ref, store):
    me = flags[2]
    for k in range(4):
        rows = pl.ds(pl.multiple_of((me ^ k) * PIECE, PIECE), PIECE)
        f_ref[rows, :] = pieces[k][...].astype(F32)
    for n in range(TC // 256):
        cols = slice(256 * n, 256 * (n + 1))
        add = jnp.dot(mix_t_ref[...], f_ref[:, cols].astype(BF16), preferred_element_type=F32)
        store(cols, (res_ref[:, cols].astype(F32) + add).astype(BF16))


def final_first_kernel(flags, p0, p1, p2, p3, res_ref, mix_t_ref, out_ref, f_ref):
    def store(cols, x):
        out_ref[:, cols] = x

    tokens_out(flags, (p0, p1, p2, p3), res_ref, mix_t_ref, f_ref, store)


def final_second_kernel(flags, p0, p1, p2, p3, res_ref, mix_t_ref, early_ref, out_ref, f_ref):
    out_ref[:, 0:TC] = early_ref[...]

    def store(cols, x):
        out_ref[:, cols.start + TC : cols.stop + TC] = x

    tokens_out(flags, (p0, p1, p2, p3), res_ref, mix_t_ref, f_ref, store)


def swap(x, k):
    return lax.ppermute(x, "chan", [(i, i ^ k) for i in range(4)])


def shards(
    tokens, filter_spectrum, skip_weight, norm_gain, mlp_gain, mix_in, up_weight, down_weight, mix_out
):
    return block(
        tokens, filter_spectrum, skip_weight[None], norm_gain[None], mlp_gain[None], mix_in,
        up_weight, down_weight, mix_out,
    )


def block(
    tokens, filter_spectrum, skip_weight, norm_gain, mlp_gain, mix_in, up_weight, down_weight, mix_out
):
    place = lax.axis_index("seq")
    lane_of = lax.axis_index("chan")
    high = place >= 32
    first = (place == 0) | (place == 63)
    flags = jnp.stack([high, first, lane_of, place]).astype(jnp.int32)
    mine = jnp.where(high, HALF, 0)
    sums = call(sums_kernel, shape((2, TOK), F32), "v")(tokens)
    others = []
    for k in (1, 2, 3):
        others.append(swap(sums, k))
    own = lax.dynamic_slice_in_dim(filter_spectrum, mine, HALF, 1)
    pick_row = jnp.arange(TOK, dtype=jnp.int32)[:, None]
    pick_col = jnp.arange(NSEQ, dtype=jnp.int32)[None, :]
    pick = (pick_row == SHARE * pick_col).astype(BF16)
    column = jnp.einsum(
        "pcj,jg->pcg", filter_spectrum.astype(BF16), pick, preferred_element_type=F32
    ).astype(BF16)
    ca = lax.ppermute(column[:, :HALF], "seq", [(32, 0)] + [(64 - i, i) for i in range(1, 32)])
    cb = lax.ppermute(column[:, HALF:], "seq", [(32, 63)] + [(i + 1, i) for i in range(32, 63)])
    freq = jnp.arange(TOK // 2, dtype=jnp.int32)
    step = jnp.arange(SHARE, dtype=jnp.int32)
    angle = (freq[None, :] * (64 * step[:, None] + place) % LENGTH).astype(F32) * (
        2.0 * math.pi / LENGTH
    )
    parity = 1.0 - 2.0 * (step % 2).astype(F32)
    beta = jnp.stack(
        [jnp.cos(angle), jnp.where(freq[None, :] == 0, -parity[:, None], jnp.sin(angle))]
    )
    turn = (
        (jnp.arange(NSEQ, dtype=jnp.int32)[:, None] * (jnp.arange(128, dtype=jnp.int32)[None, :])) % 64
    ).astype(F32) * (2.0 * math.pi / 64)
    alpha = jnp.stack([jnp.cos(turn), jnp.sin(turn)])
    table, give = call(
        table_kernel, (shape((TOK, TOK), BF16), shape((2, HALF, TOK), BF16)), "svvh",
        scratch=[pltpu.VMEM((2, HALF, TOK), F32), pltpu.SemaphoreType.DMA(())],
    )(flags, alpha, beta, in_hbm(filter_spectrum))
    got = lax.ppermute(give, "seq", [(i, 63 - i) for i in range(64)])
    send, normed = call(
        forward_kernel,
        (shape((NSEQ, 2 * QUART, 128), BF16), shape((CH, TOK), BF16)),
        "v" * 7,
        mib=20,
    )(tokens, sums, *others, norm_gain, table)
    moved = lax.all_to_all(send, "seq", split_axis=0, concat_axis=0, tiled=True)
    gains, gains_first = call(
        filter_kernel,
        (pltpu.HBM((2, NSEQ, QUART, 128), F32), pltpu.HBM((2, NSEQ, QUART, 128), F32)),
        "svvvv",
        scratch=[
            pltpu.VMEM((2, NSEQ, QUART, 128), F32),
            pltpu.VMEM((2, NSEQ, QUART, 128), F32),
            pltpu.SemaphoreType.DMA((3,)),
        ],
        outs="hh",
    )(flags, own, got, ca, cb)
    mix_in_full, mix_in_t, up_t, down_t, mix_out_t = call(
        weights_kernel,
        (
            shape((CH, CH), BF16), shape((CH, CH), BF16), shape((HID, CH), BF16),
            shape((CH, HID), BF16), shape((CH, CH), BF16),
        ),
        "vvvv",
        scratch=[pltpu.VMEM((CH, CH), F32), pltpu.VMEM((CH, HID), F32), pltpu.VMEM((HID, CH), F32)],
    )(mix_in, up_weight, down_weight, mix_out)
    moved, mix_in_full, mix_in_t, down_t, up_t, mix_out_t = lax.optimization_barrier(
        (moved, mix_in_full, mix_in_t, down_t, up_t, mix_out_t)
    )
    back = call(
        middle_kernel,
        shape((NSEQ, 2 * QUART, 128), BF16),
        "svhh",
        scratch=[
            pltpu.VMEM((NSEQ, 2 * QUART, 128), F32),
            pltpu.VMEM((2, NSEQ, 8, 128), F32),
            pltpu.VMEM((2, NSEQ, 8, 128), F32),
            pltpu.VMEM((NSEQ, QUART, 128), F32),
            pltpu.VMEM((2, NSEQ, QUART, 128), F32),
            pltpu.VMEM((2, NSEQ, QUART, 128), F32),
            pltpu.SemaphoreType.DMA((2,)),
        ],
    )(flags, moved, in_hbm(gains), in_hbm(gains_first))
    home = lax.all_to_all(back, "seq", split_axis=0, concat_axis=0, tiled=True)
    piece = (shape((CH, TC), BF16),) + (shape((ROWS, TC), BF16),) * 4
    small = [
        pltpu.VMEM((CH, TC), F32),
        pltpu.VMEM((8, TC), F32),
        pltpu.VMEM((TC, TOK), BF16),
        pltpu.SemaphoreType.DMA((TC // 256,)),
    ]
    rest = (in_hbm(table), tokens, normed, skip_weight, mlp_gain, mix_in_full, mix_in_t)
    values, res_a, *first_a = call(
        back_first_kernel, (shape((CH, TOK), BF16),) + piece, "svhvvvvvv",
        scratch=[pltpu.VMEM((CH, TOK), F32)] + small, mib=20,
    )(flags, home, *rest)
    arrived_a = [first_a[0]] + [swap(first_a[k], k) for k in (1, 2, 3)]
    res_b, *first_b = call(
        back_second_kernel, piece, "svhvvvvvv", scratch=small, mib=20
    )(flags, values, *rest)
    arrived_b = [first_b[0]] + [swap(first_b[k], k) for k in (1, 2, 3)]

    def mlp(arrived):
        lows = call(
            mlp_kernel,
            (shape((PIECE, TC), BF16),) * 4,
            "s" + "v" * 6,
            scratch=[pltpu.VMEM((CH, TC), F32), pltpu.VMEM((CH, TC), F32)],
        )(flags, *arrived, up_t, down_t)
        return [lows[0]] + [swap(lows[k], k) for k in (1, 2, 3)]

    back_home_a = mlp(arrived_a)
    back_home_b = mlp(arrived_b)
    early = call(
        final_first_kernel, shape((CH, TC), BF16), "s" + "v" * 6, scratch=[pltpu.VMEM((CH, TC), F32)],
    )(flags, *back_home_a, res_a, mix_out_t)
    return call(
        final_second_kernel, shape((CH, TOK), BF16), "s" + "v" * 7, scratch=[pltpu.VMEM((CH, TC), F32)],
    )(flags, *back_home_b, res_b, mix_out_t, early)


def solution(mesh):
    in_specs = (
        P("chan", "seq"),
        P(None, "chan", "seq"),
        P("chan"),
        P("chan"),
        P("chan"),
        P("chan", None),
        P("chan", None),
        P("chan", None),
        P("chan", None),
    )
    out_specs = P("chan", "seq")
    return jax.shard_map(shards, mesh=mesh, in_specs=in_specs, out_specs=out_specs, check_vma=False)
```

```python
import math

import jax
import jax.numpy as jnp
from jax import lax
from jax.experimental import pallas as pl
from jax.experimental.pallas import tpu as pltpu
from jax.sharding import PartitionSpec as P


D = 768
CH = 192
HALF = 96
QUART = 24
TOK = 2048
NSEQ = 64
SHARE = 32
LENGTH = TOK * NSEQ
HID = 768
PIECE = 48
CHUNKS = 2
TC = TOK // CHUNKS
F32 = jnp.float32
BF16 = jnp.bfloat16
ROOT_HALF = math.sqrt(0.5)
MIB = 1024 * 1024
ROWS = 56


def vm():
    return pl.BlockSpec(memory_space=pltpu.VMEM)


def sm():
    return pl.BlockSpec(memory_space=pltpu.SMEM)


def hb():
    return pl.BlockSpec(memory_space=pltpu.HBM)


def call(body, out_shape, kinds, scratch=(), mib=14, outs=None):
    spec = {"s": sm, "v": vm, "h": hb}
    many = isinstance(out_shape, (tuple, list))
    outs = outs or "v" * (len(out_shape) if many else 1)
    return pl.pallas_call(
        body,
        out_shape=out_shape,
        in_specs=[spec[k]() for k in kinds],
        out_specs=[spec[k]() for k in outs] if many else spec[outs](),
        scratch_shapes=scratch,
        compiler_params=pltpu.CompilerParams(vmem_limit_bytes=mib * MIB),
    )


def in_hbm(x):
    return pltpu.with_memory_space_constraint(x, pltpu.HBM)


def shape(dims, dtype):
    return jax.ShapeDtypeStruct(dims, dtype)


def lane_group(rows):
    return lax.broadcasted_iota(jnp.int32, (rows, 128), 1)


def regroup(parts):
    lane = lane_group(parts[0].shape[0])
    step = list(parts)
    bit = len(parts) // 2
    while bit:
        d = 16 * bit
        low = (lane // d) % 2 == 0
        for a in range(len(parts)):
            if a & bit:
                continue
            x, y = step[a], step[a | bit]
            step[a] = jnp.where(low, x, pltpu.roll(y, d, 1))
            step[a | bit] = jnp.where(low, pltpu.roll(x, 128 - d, 1), y)
        bit //= 2
    return step


def column_of(row_ref):
    n = row_ref.shape[1]
    eye = lax.broadcasted_iota(jnp.int32, (n, n), 0) == lax.broadcasted_iota(jnp.int32, (n, n), 1)
    return jnp.sum(jnp.where(eye, row_ref[...], 0.0), axis=1, keepdims=True)


def sums_kernel(x_ref, out_ref):
    x = x_ref[...].astype(F32)
    out_ref[0:1, :] = jnp.sum(x, axis=0, keepdims=True)
    out_ref[1:2, :] = jnp.sum(x * x, axis=0, keepdims=True)


def give_kernel(flags, filter_ref, give_ref, held, ready, sems, out_sems):
    theirs = pl.multiple_of((1 - flags[0]) * HALF, HALF)
    rows = 32
    fetches = []
    for n in range(6):
        part, k = n // 3, n % 3
        fetches.append(
            pltpu.make_async_copy(
                filter_ref.at[part, pl.ds(theirs + rows * k, rows), :], held.at[n], sems.at[n]
            )
        )
        fetches[-1].start()
    sends = []
    for n in range(6):
        part, k = n // 3, n % 3
        fetches[n].wait()
        ready[n] = held[n].astype(BF16)
        sends.append(
            pltpu.make_async_copy(
                ready.at[n], give_ref.at[part, rows * k : rows * (k + 1), :], out_sems.at[n]
            )
        )
        sends[-1].start()
    for send in sends:
        send.wait()


def table_kernel(alpha_ref, beta_ref, w_ref):
    def rows(b, carry):
        start = pl.multiple_of(b * SHARE, SHARE)
        for par in range(2):
            ac = jnp.broadcast_to(alpha_ref[0, pl.ds(b + 32 * par, 1), :], (SHARE, 128))
            as_ = jnp.broadcast_to(alpha_ref[1, pl.ds(b + 32 * par, 1), :], (SHARE, 128))
            for u in range(4 * par, 4 * par + 4):
                bc = beta_ref[0, :, 128 * u : 128 * (u + 1)]
                bs = beta_ref[1, :, 128 * u : 128 * (u + 1)]
                w_ref[pl.ds(start, SHARE), 256 * u : 256 * u + 128] = (ac * bc - as_ * bs).astype(
                    BF16
                )
                w_ref[pl.ds(start, SHARE), 256 * u + 128 : 256 * (u + 1)] = (
                    -(as_ * bc + ac * bs)
                ).astype(BF16)
        return carry

    lax.fori_loop(0, 32, rows, 0)


def forward_kernel(
    x_ref, s0, s1, s2, s3, gain_ref, w_ref, send_ref, normed_ref, kept_ref, fold, sem
):
    keep = pltpu.make_async_copy(w_ref, kept_ref, sem)
    keep.start()
    total = s0[...] + s1[...] + s2[...] + s3[...]
    mean = total[0:1, :] / D
    square = total[1:2, :] / D
    scale = lax.rsqrt(square - mean * mean + 1e-05)
    xn = ((x_ref[...].astype(F32) - mean) * scale * column_of(gain_ref)).astype(BF16)
    normed_ref[...] = xn
    left = xn[:, : TOK // 2].astype(F32)
    right = xn[:, TOK // 2 :].astype(F32)
    fold[0] = (left + right).astype(BF16)
    fold[1] = (left - right).astype(BF16)
    for b in range(4):
        y = [
            jnp.dot(
                fold[par],
                w_ref[:, 1024 * par + 256 * b : 1024 * par + 256 * (b + 1)],
                preferred_element_type=F32,
            )
            for par in range(2)
        ]
        for half in range(2):
            both = []
            for part in range(2):
                both.append(
                    regroup(
                        [
                            y[par][
                                half * HALF + w * QUART : half * HALF + (w + 1) * QUART,
                                128 * part : 128 * (part + 1),
                            ]
                            for par in range(2)
                            for w in range(4)
                        ]
                    )
                )
            for v in range(8):
                q = 8 * b + v
                dest = 63 - q if half else q
                send_ref[dest] = jnp.concatenate([both[0][v], both[1][v]], axis=0).astype(BF16)
    keep.wait()


def lanes_of(rows):
    lane = lax.broadcasted_iota(jnp.int32, (rows, 128), 1)
    group = (lane // 16) % 4
    return 2 * (lane % 16) + lane // 64, group


def make_gains(flags, own_ref, got_ref, ca_ref, cb_ref, g_ref, g1_ref):
    high = flags[0] == 1
    first = flags[1] == 1
    row = lax.broadcasted_iota(jnp.int32, (128, 128), 0)
    freq, group = lanes_of(128)
    lane = SHARE * group + freq
    straight = jnp.where(row == lane, 1.0, 0.0)
    mirror = jnp.where((row + lane == 128) & (freq != 0), 1.0, 0.0)
    crow = lax.broadcasted_iota(jnp.int32, (NSEQ, 128), 0)
    cfreq, cgroup = lanes_of(NSEQ)
    keep = jnp.where(first, 0.0, 1.0)

    def column(part):
        return (ca_ref[part].astype(F32) + cb_ref[part].astype(F32)).astype(BF16)

    for part in range(2):
        sign = 1.0 if part == 0 else -1.0
        maps = jnp.concatenate([straight, sign * mirror], axis=0).astype(BF16)
        crossed = jnp.concatenate(
            [
                jnp.where((cfreq == 0) & (crow == 63 - 4 * t - cgroup), sign * keep, 0.0)
                for t in range(16)
            ],
            axis=1,
        ).astype(BF16)
        extra = jnp.dot(column(part), crossed, preferred_element_type=F32)
        own = own_ref[part]
        got = got_ref[part]
        direct = jnp.where(high, got, own)
        other = jnp.where(high, own, got)
        for t in range(16):
            pair = jnp.concatenate(
                [direct[:, 128 * t : 128 * (t + 1)], other[:, 128 * (15 - t) : 128 * (16 - t)]],
                axis=1,
            )
            both = (
                jnp.dot(pair, maps, preferred_element_type=F32)
                + extra[:, 128 * t : 128 * (t + 1)]
            )
            out = regroup([both[w * QUART : (w + 1) * QUART] for w in range(4)])
            for v in range(4):
                g_ref[part, 4 * t + v] = out[v]

    @pl.when(first)
    def _():
        for part in range(2):
            plain = jnp.concatenate(
                [
                    jnp.where((cfreq == 0) & (crow == 4 * t + cgroup), 1.0, 0.0)
                    for t in range(16)
                ],
                axis=1,
            ).astype(BF16)
            alone = jnp.dot(column(part), plain, preferred_element_type=F32)
            for t in range(16):
                both = alone[:, 128 * t : 128 * (t + 1)]
                out = regroup([both[w * QUART : (w + 1) * QUART] for w in range(4)])
                for v in range(4):
                    g1_ref[part, 4 * t + v] = packed([out[v][8 * k : 8 * k + 8] for k in range(3)])


def packed(tiles):
    return tiles[0] + pltpu.roll(tiles[1], 1, 1) + pltpu.roll(tiles[2], 2, 1)


def turn_i(re, im, s):
    return (-im, re) if s > 0 else (im, -re)


def dft4(xr, xi, s):
    ar, ai = xr[0] + xr[2], xi[0] + xi[2]
    br, bi = xr[0] - xr[2], xi[0] - xi[2]
    cr, ci = xr[1] + xr[3], xi[1] + xi[3]
    dr, di = turn_i(xr[1] - xr[3], xi[1] - xi[3], s)
    return [ar + cr, br + dr, ar - cr, br - dr], [ai + ci, bi + di, ai - ci, bi - di]


def dft8(xr, xi, s):
    er, ei = dft4(xr[0::2], xi[0::2], s)
    dr, di = dft4(xr[1::2], xi[1::2], s)
    c = ROOT_HALF
    if s > 0:
        dr1, di1 = c * (dr[1] - di[1]), c * (di[1] + dr[1])
        dr3, di3 = -c * (dr[3] + di[3]), c * (dr[3] - di[3])
    else:
        dr1, di1 = c * (dr[1] + di[1]), c * (di[1] - dr[1])
        dr3, di3 = c * (di[3] - dr[3]), -c * (di[3] + dr[3])
    dr2, di2 = turn_i(dr[2], di[2], s)
    qr = [dr[0], dr1, dr2, dr3]
    qi = [di[0], di1, di2, di3]
    return (
        [er[k] + qr[k] for k in range(4)] + [er[k] - qr[k] for k in range(4)],
        [ei[k] + qi[k] for k in range(4)] + [ei[k] - qi[k] for k in range(4)],
    )


def twiddle(re, im, index, s):
    index %= 64
    if index == 0:
        return re, im
    c = math.cos(2.0 * math.pi * index / 64.0)
    d = s * math.sin(2.0 * math.pi * index / 64.0)
    return re * c - im * d, im * c + re * d


def across(load, store, gains, a_ref, b_ref):
    for p0 in range(8):
        xr, xi = zip(*[load(p0 + 8 * p1) for p1 in range(8)])
        yr, yi = dft8(list(xr), list(xi), -1)
        for g1 in range(8):
            a_ref[0, g1 * 8 + p0], a_ref[1, g1 * 8 + p0] = twiddle(yr[g1], yi[g1], p0 * g1, -1)
    for g1 in range(8):
        yr, yi = dft8(
            [a_ref[0, g1 * 8 + p0] for p0 in range(8)],
            [a_ref[1, g1 * 8 + p0] for p0 in range(8)],
            -1,
        )
        for g2 in range(8):
            hr, hi = gains(g1 + 8 * g2)
            yr[g2], yi[g2] = hr * yr[g2] - hi * yi[g2], hr * yi[g2] + hi * yr[g2]
        zr, zi = dft8(yr, yi, 1)
        for p0 in range(8):
            b_ref[0, p0 * 8 + g1], b_ref[1, p0 * 8 + g1] = twiddle(zr[p0], zi[p0], g1 * p0, 1)
    for p0 in range(8):
        zr, zi = dft8(
            [b_ref[0, p0 * 8 + g1] for g1 in range(8)],
            [b_ref[1, p0 * 8 + g1] for g1 in range(8)],
            1,
        )
        for p1 in range(8):
            store(p0 + 8 * p1, zr[p1], zi[p1])


def middle_kernel(
    flags, moved, own_ref, got, ca_ref, cb_ref, out_ref,
    moved_ref, got_ref, g_ref, g1_ref, xs, a_ref, b_ref, t1, sems,
):
    first = flags[1] == 1
    fetches = [
        pltpu.make_async_copy(got, got_ref, sems.at[0]),
        pltpu.make_async_copy(moved, moved_ref, sems.at[1]),
    ]
    for fetch in fetches:
        fetch.start()
    freq, _ = lanes_of(8)
    special = (freq == 0) & first
    fetches[0].wait()
    make_gains(flags, own_ref, got_ref, ca_ref, cb_ref, g_ref, g1_ref)
    fetches[1].wait()

    def widen(p, carry):
        xs[p] = moved_ref[p].astype(F32)
        return carry

    lax.fori_loop(0, NSEQ, widen, 0, unroll=8)

    def half_turn(p):
        return math.cos(2.0 * math.pi * p / 128.0), math.sin(2.0 * math.pi * p / 128.0)

    @pl.when(first)
    def _():
        def load(p):
            c, s = half_turn(p)
            im = packed(
                [
                    jnp.where(special, xs[p, QUART + 8 * k : QUART + 8 * k + 8, :], 0.0)
                    for k in range(3)
                ]
            )
            return im * c, im * (-s)

        def store(p, re, im):
            c, s = half_turn(p)
            turned = re * c - im * s
            t1[p, 0:8, :] = turned
            t1[p, 8:16, :] = pltpu.roll(turned, 127, 1)
            t1[p, 16:24, :] = pltpu.roll(turned, 126, 1)

        across(load, store, lambda g: (g1_ref[0, g], g1_ref[1, g]), a_ref, b_ref)

    def every(i, carry):
        top = pl.ds(pl.multiple_of(i * 8, 8), 8)
        bottom = pl.ds(pl.multiple_of(i * 8 + QUART, 8), 8)

        def load(p):
            return xs[p, top, :], jnp.where(special, 0.0, xs[p, bottom, :])

        def store(p, re, im):
            xs[p, top, :] = re
            xs[p, bottom, :] = jnp.where(special, t1[p, top, :], im)

        across(load, store, lambda g: (g_ref[0, g, top, :], g_ref[1, g, top, :]), a_ref, b_ref)
        return carry

    lax.fori_loop(0, 3, every, 0)

    def narrow(p, carry):
        out_ref[p] = xs[p].astype(BF16)
        return carry

    lax.fori_loop(0, NSEQ, narrow, 0, unroll=8)


def in_three(x):
    a = x.astype(BF16)
    rest = x - a.astype(F32)
    b = rest.astype(BF16)
    return [a, b, (rest - b.astype(F32)).astype(BF16)]


def tokens_back(
    flags, values, w_ref, x_ref, normed_ref, skip_row, gain_row, mix_ref, mix_t_ref, res_ref, outs, tm, st,
    fetches,
    chunk,
):
    me = flags[2]
    skip = column_of(skip_row)
    gain = column_of(gain_row)
    st[...] = jnp.zeros((8, TC), F32)
    weight = jnp.dot(
        gain_row[...], mix_ref[...].astype(F32), preferred_element_type=F32,
        precision=lax.Precision.HIGHEST,
    )
    for k, part in enumerate(in_three(weight)[:2]):
        st[5 + k : 6 + k, 0:CH] = part.astype(F32)
    for n in range(TC // 512):
        mine = slice(256 * n, 256 * (n + 1))
        fetches[n].wait()
        even, odd = (
            lax.dot_general(
                values[:, 1024 * par : 1024 * (par + 1)],
                w_ref[mine, 1024 * par : 1024 * (par + 1)],
                (((1,), (1,)), ((), ())),
                preferred_element_type=F32,
            )
            for par in range(2)
        )
        for side, conv in enumerate((even + odd, even - odd)):
            here = slice(side * TC // 2 + 256 * n, side * TC // 2 + 256 * (n + 1))
            start = side * TOK // 2 + chunk * TC // 2 + 256 * n
            cols = slice(start, start + 256)
            res = (
                x_ref[:, cols].astype(F32)
                + conv * (1.0 / LENGTH)
                + skip * normed_ref[:, cols].astype(F32)
            ).astype(BF16)
            res_ref[:, here] = res
            r = res.astype(F32)
            mean = jnp.sum(r, axis=0, keepdims=True) * (1.0 / CH)
            centred = r - mean
            for k, part in enumerate(in_three(mean)):
                st[k : k + 1, here] = part.astype(F32)
            for k, part in enumerate(
                in_three(jnp.sum(centred * centred, axis=0, keepdims=True))[:2]
            ):
                st[3 + k : 4 + k, here] = part.astype(F32)
            z = (centred * gain).astype(BF16)
            tm[:, here] = jnp.dot(mix_t_ref[...], z, preferred_element_type=F32)
    for k in range(4):
        rows = pl.ds(pl.multiple_of((me ^ k) * PIECE, PIECE), PIECE)
        outs[k][...] = jnp.concatenate([tm[rows, :], st[...]], axis=0).astype(BF16)


def fetch_table(w_hbm, w_ref, sems, chunk):
    fetches = []
    for n in range(TC // 512):
        here = slice(256 * n, 256 * (n + 1))
        there = slice(chunk * TC // 2 + 256 * n, chunk * TC // 2 + 256 * (n + 1))
        fetches.append(pltpu.make_async_copy(w_hbm.at[there, :], w_ref.at[here, :], sems.at[n]))
        fetches[-1].start()
    return fetches


def back_first_kernel(
    flags, got_ref, w_hbm, x_ref, normed_ref, skip_row, gain_row, mix_ref, mix_t_ref,
    values_ref, res_ref, u0, u1, u2, u3, tall, tm, st, w_ref, sems,
):
    fetches = fetch_table(w_hbm, w_ref, sems, 0)
    for half in range(2):
        for b in range(4):
            parts = []
            for v in range(8):
                q = 8 * b + v
                parts.append(got_ref[63 - q if half else q].astype(F32))
            out = regroup(parts)
            for k in range(8):
                low = half * HALF + (k % 4) * QUART
                left = 1024 * (k // 4) + 256 * b
                tall[low : low + QUART, left : left + 128] = out[k][:QUART]
                tall[low : low + QUART, left + 128 : left + 256] = out[k][QUART:]
    values = tall[...].astype(BF16)
    values_ref[...] = values
    tokens_back(
        flags, values_ref[...], w_ref, x_ref, normed_ref, skip_row, gain_row, mix_ref, mix_t_ref, res_ref,
        (u0, u1, u2, u3), tm, st, fetches, 0,
    )


def back_second_kernel(
    flags, values_ref, w_hbm, x_ref, normed_ref, skip_row, gain_row, mix_ref, mix_t_ref,
    res_ref, u0, u1, u2, u3, tm, st, w_ref, sems,
):
    fetches = fetch_table(w_hbm, w_ref, sems, 1)
    tokens_back(
        flags, values_ref[...], w_ref, x_ref, normed_ref, skip_row, gain_row, mix_ref, mix_t_ref, res_ref,
        (u0, u1, u2, u3), tm, st, fetches, 1,
    )


def mlp_kernel(flags, p0, p1, p2, p3, up_t, down_t, o0, o1, o2, o3, f_ref, low_ref):
    me = flags[2]
    values = [p[...].astype(F32) for p in (p0, p1, p2, p3)]
    tails = [x[PIECE:ROWS] for x in values]
    means = [t[0:1] + t[1:2] + t[2:3] for t in tails]
    mean = (means[0] + means[1] + means[2] + means[3]) * 0.25
    spread = sum(t[3:4] + t[4:5] for t in tails) + CH * sum((m - mean) * (m - mean) for m in means)
    scale = lax.rsqrt(spread * (1.0 / D) + 1e-05)
    row = lax.broadcasted_iota(jnp.int32, (PIECE, CH), 0)
    lane = lax.broadcasted_iota(jnp.int32, (PIECE, CH), 1)
    pick = lane == row + me * PIECE
    for k in range(4):
        line = tails[k][5:6, 0:CH] + tails[k][6:7, 0:CH]
        weight = jnp.sum(jnp.where(pick, line, 0.0), axis=1, keepdims=True)
        f_ref[pl.ds(pl.multiple_of((me ^ k) * PIECE, PIECE), PIECE), :] = scale * (
            values[k][:PIECE] - (mean - means[k]) * weight
        )
    for n in range(TC // 256):
        cols = slice(256 * n, 256 * (n + 1))
        f = f_ref[:, cols].astype(BF16)
        total = None
        for h in range(3):
            rows = slice(256 * h, 256 * (h + 1))
            wide = jnp.dot(up_t[rows, :], f, preferred_element_type=F32)
            act = (0.5 * wide * (1.0 + lax.erf(wide * ROOT_HALF))).astype(BF16)
            part = jnp.dot(down_t[:, rows], act, preferred_element_type=F32)
            total = part if total is None else total + part
        low_ref[:, cols] = total
    for k, o in enumerate((o0, o1, o2, o3)):
        o[...] = low_ref[pl.ds(pl.multiple_of((me ^ k) * PIECE, PIECE), PIECE), :].astype(BF16)


def weights_kernel(
    mix_in_ref, up_ref, down_ref, mix_out_ref, in_ref, in_t, up_t, down_t, out_t, square, wide, tall
):
    def unroll(src, dst, rows, cols):
        def step(i, carry):
            for k in range(8):
                row = i * 8 + k
                start = pl.multiple_of(row * cols, 128)
                dst[pl.ds(row, 1), :] = src[:, pl.ds(start, cols)].astype(F32)
            return carry

        lax.fori_loop(0, rows // 8, step, 0)

    unroll(up_ref, wide, CH, HID)
    up_t[...] = wide[...].T.astype(BF16)
    for src, dst in ((mix_in_ref, in_t), (mix_out_ref, out_t)):
        paired(src, square, CH)
        if dst is in_t:
            in_ref[...] = square[...].astype(BF16)
        dst[...] = square[...].T.astype(BF16)
    paired(down_ref, tall, HID)
    down_t[...] = tall[...].T.astype(BF16)


def paired(src, dst, rows):
    def step(i, carry):
        for k in range(4):
            row = i * 8 + 2 * k
            start = pl.multiple_of(row * CH, 128)
            both = src[:, pl.ds(start, 2 * CH)].astype(F32)
            dst[pl.ds(row, 1), :] = both[:, :CH]
            dst[pl.ds(row + 1, 1), :] = both[:, CH:]
        return carry

    lax.fori_loop(0, rows // 8, step, 0)


def tokens_out(flags, pieces, res_ref, mix_t_ref, f_ref, store):
    me = flags[2]
    for k in range(4):
        rows = pl.ds(pl.multiple_of((me ^ k) * PIECE, PIECE), PIECE)
        f_ref[rows, :] = pieces[k][...].astype(F32)
    for n in range(TC // 256):
        cols = slice(256 * n, 256 * (n + 1))
        add = jnp.dot(mix_t_ref[...], f_ref[:, cols].astype(BF16), preferred_element_type=F32)
        store(cols, (res_ref[:, cols].astype(F32) + add).astype(BF16))


def final_first_kernel(flags, p0, p1, p2, p3, res_ref, mix_t_ref, out_ref, f_ref):
    def store(cols, x):
        out_ref[:, cols] = x

    tokens_out(flags, (p0, p1, p2, p3), res_ref, mix_t_ref, f_ref, store)


def final_second_kernel(flags, p0, p1, p2, p3, res_ref, mix_t_ref, early_ref, out_ref, f_ref):
    side = TC // 2
    for k in range(2):
        out_ref[:, 2 * k * side : (2 * k + 1) * side] = early_ref[:, k * side : (k + 1) * side]

    def store(cols, x):
        start = cols.start + (side if cols.start < side else 2 * side)
        out_ref[:, start : start + 256] = x

    tokens_out(flags, (p0, p1, p2, p3), res_ref, mix_t_ref, f_ref, store)


def swap(x, k):
    return lax.ppermute(x, "chan", [(i, i ^ k) for i in range(4)])


def shards(
    tokens, filter_spectrum, skip_weight, norm_gain, mlp_gain, mix_in, up_weight, down_weight, mix_out
):
    return block(
        tokens, filter_spectrum, skip_weight[None], norm_gain[None], mlp_gain[None], mix_in,
        up_weight, down_weight, mix_out,
    )


def block(
    tokens, filter_spectrum, skip_weight, norm_gain, mlp_gain, mix_in, up_weight, down_weight, mix_out
):
    place = lax.axis_index("seq")
    lane_of = lax.axis_index("chan")
    high = place >= 32
    first = (place == 0) | (place == 63)
    flags = jnp.stack([high, first, lane_of, place]).astype(jnp.int32)
    mine = jnp.where(high, HALF, 0)
    give = call(
        give_kernel, pltpu.HBM((2, HALF, TOK), BF16), "sh",
        scratch=[
            pltpu.VMEM((6, 32, TOK), F32), pltpu.VMEM((6, 32, TOK), BF16),
            pltpu.SemaphoreType.DMA((6,)), pltpu.SemaphoreType.DMA((6,)),
        ],
        outs="h",
    )(flags, in_hbm(filter_spectrum))
    got = lax.ppermute(give, "seq", [(i, 63 - i) for i in range(64)])
    sums = call(sums_kernel, shape((2, TOK), F32), "v")(tokens)
    others = []
    for k in (1, 2, 3):
        others.append(swap(sums, k))
    own = lax.dynamic_slice_in_dim(filter_spectrum, mine, HALF, 1).astype(BF16)
    pick_row = jnp.arange(TOK, dtype=jnp.int32)[:, None]
    pick_col = jnp.arange(NSEQ, dtype=jnp.int32)[None, :]
    pick = (pick_row == SHARE * pick_col).astype(BF16)
    column = jnp.einsum(
        "pcj,jg->pcg", filter_spectrum.astype(BF16), pick, preferred_element_type=F32
    ).astype(BF16)
    ca = lax.ppermute(column[:, :HALF], "seq", [(32, 0)] + [(64 - i, i) for i in range(1, 32)])
    cb = lax.ppermute(column[:, HALF:], "seq", [(32, 63)] + [(i + 1, i) for i in range(32, 63)])
    slot = jnp.arange(TOK // 2, dtype=jnp.int32)
    freq = 256 * (slot // 128 % 4) + 2 * (slot % 128) + slot // 512
    step = jnp.arange(SHARE, dtype=jnp.int32)
    angle = (freq[None, :] * (64 * step[:, None] + place) % LENGTH).astype(F32) * (
        2.0 * math.pi / LENGTH
    )
    parity = 1.0 - 2.0 * (step % 2).astype(F32)
    beta = jnp.stack(
        [jnp.cos(angle), jnp.where(freq[None, :] == 0, -parity[:, None], jnp.sin(angle))]
    )
    half_row = jnp.arange(64, dtype=jnp.int32)[:, None]
    half_freq = 2 * jnp.arange(128, dtype=jnp.int32)[None, :] + half_row // 32
    turn = ((half_row % 32) * half_freq % 64).astype(F32) * (2.0 * math.pi / 64)
    alpha = jnp.stack([jnp.cos(turn), jnp.sin(turn)])
    table = call(table_kernel, shape((TOK // 2, TOK), BF16), "vv")(alpha, beta)
    send, normed, kept = call(
        forward_kernel,
        (
            shape((NSEQ, 2 * QUART, 128), BF16),
            shape((CH, TOK), BF16),
            pltpu.HBM((TOK // 2, TOK), BF16),
        ),
        "v" * 7,
        scratch=[pltpu.VMEM((2, CH, TOK // 2), BF16), pltpu.SemaphoreType.DMA(())],
        outs="vvh",
        mib=20,
    )(tokens, sums, *others, norm_gain, table)
    moved = lax.all_to_all(send, "seq", split_axis=0, concat_axis=0, tiled=True)
    back = call(
        middle_kernel,
        shape((NSEQ, 2 * QUART, 128), BF16),
        "shvhvv",
        scratch=[
            pltpu.VMEM((NSEQ, 2 * QUART, 128), BF16),
            pltpu.VMEM((2, HALF, TOK), BF16),
            pltpu.VMEM((2, NSEQ, QUART, 128), F32),
            pltpu.VMEM((2, NSEQ, 8, 128), F32),
            pltpu.VMEM((NSEQ, 2 * QUART, 128), F32),
            pltpu.VMEM((2, NSEQ, 8, 128), F32),
            pltpu.VMEM((2, NSEQ, 8, 128), F32),
            pltpu.VMEM((NSEQ, QUART, 128), F32),
            pltpu.SemaphoreType.DMA((2,)),
        ],
    )(flags, in_hbm(moved), own, in_hbm(got), ca, cb)
    back, mix_in, up_weight, down_weight, mix_out = lax.optimization_barrier(
        (back, mix_in, up_weight, down_weight, mix_out)
    )
    mix_in_full, mix_in_t, up_t, down_t, mix_out_t = call(
        weights_kernel,
        (
            shape((CH, CH), BF16), shape((CH, CH), BF16), shape((HID, CH), BF16),
            shape((CH, HID), BF16), shape((CH, CH), BF16),
        ),
        "vvvv",
        scratch=[pltpu.VMEM((CH, CH), F32), pltpu.VMEM((CH, HID), F32), pltpu.VMEM((HID, CH), F32)],
    )(mix_in, up_weight, down_weight, mix_out)
    home = lax.all_to_all(back, "seq", split_axis=0, concat_axis=0, tiled=True)
    home, mix_in_full, mix_in_t, down_t, up_t, mix_out_t = lax.optimization_barrier(
        (home, mix_in_full, mix_in_t, down_t, up_t, mix_out_t)
    )
    piece = (shape((CH, TC), BF16),) + (shape((ROWS, TC), BF16),) * 4
    small = [
        pltpu.VMEM((CH, TC), F32),
        pltpu.VMEM((8, TC), F32),
        pltpu.VMEM((TC // 2, TOK), BF16),
        pltpu.SemaphoreType.DMA((TC // 512,)),
    ]
    rest = (in_hbm(kept), tokens, normed, skip_weight, mlp_gain, mix_in_full, mix_in_t)
    values, res_a, *first_a = call(
        back_first_kernel, (shape((CH, TOK), BF16),) + piece, "svhvvvvvv",
        scratch=[pltpu.VMEM((CH, TOK), F32)] + small, mib=20,
    )(flags, home, *rest)
    arrived_a = [first_a[0]] + [swap(first_a[k], k) for k in (1, 2, 3)]
    res_b, *first_b = call(
        back_second_kernel, piece, "svhvvvvvv", scratch=small, mib=20
    )(flags, values, *rest)
    arrived_b = [first_b[0]] + [swap(first_b[k], k) for k in (1, 2, 3)]

    def mlp(arrived):
        lows = call(
            mlp_kernel,
            (shape((PIECE, TC), BF16),) * 4,
            "s" + "v" * 6,
            scratch=[pltpu.VMEM((CH, TC), F32), pltpu.VMEM((CH, TC), F32)],
        )(flags, *arrived, up_t, down_t)
        return [lows[0]] + [swap(lows[k], k) for k in (1, 2, 3)]

    back_home_a = mlp(arrived_a)
    back_home_b = mlp(arrived_b)
    early = call(
        final_first_kernel, shape((CH, TC), BF16), "s" + "v" * 6, scratch=[pltpu.VMEM((CH, TC), F32)],
    )(flags, *back_home_a, res_a, mix_out_t)
    return call(
        final_second_kernel, shape((CH, TOK), BF16), "s" + "v" * 7, scratch=[pltpu.VMEM((CH, TC), F32)],
    )(flags, *back_home_b, res_b, mix_out_t, early)


def solution(mesh):
    in_specs = (
        P("chan", "seq"),
        P(None, "chan", "seq"),
        P("chan"),
        P("chan"),
        P("chan"),
        P("chan", None),
        P("chan", None),
        P("chan", None),
        P("chan", None),
    )
    out_specs = P("chan", "seq")
    return jax.shard_map(shards, mesh=mesh, in_specs=in_specs, out_specs=out_specs, check_vma=False)
```

```python
import math

import jax
import jax.numpy as jnp
from jax import lax
from jax.experimental import pallas as pl
from jax.experimental.pallas import tpu as pltpu
from jax.sharding import PartitionSpec as P


D = 768
CH = 192
HALF = 96
QUART = 24
TOK = 2048
NSEQ = 64
SHARE = 32
LENGTH = TOK * NSEQ
HID = 768
PIECE = 48
CHUNKS = 2
TC = TOK // CHUNKS
F32 = jnp.float32
BF16 = jnp.bfloat16
ROOT_HALF = math.sqrt(0.5)
MIB = 1024 * 1024
ROWS = 56


def vm():
    return pl.BlockSpec(memory_space=pltpu.VMEM)


def sm():
    return pl.BlockSpec(memory_space=pltpu.SMEM)


def hb():
    return pl.BlockSpec(memory_space=pltpu.HBM)


def call(body, out_shape, kinds, scratch=(), mib=14, outs=None):
    spec = {"s": sm, "v": vm, "h": hb}
    many = isinstance(out_shape, (tuple, list))
    outs = outs or "v" * (len(out_shape) if many else 1)
    return pl.pallas_call(
        body,
        out_shape=out_shape,
        in_specs=[spec[k]() for k in kinds],
        out_specs=[spec[k]() for k in outs] if many else spec[outs](),
        scratch_shapes=scratch,
        compiler_params=pltpu.CompilerParams(vmem_limit_bytes=mib * MIB),
    )


def in_hbm(x):
    return pltpu.with_memory_space_constraint(x, pltpu.HBM)


def shape(dims, dtype):
    return jax.ShapeDtypeStruct(dims, dtype)


def lane_group(rows):
    return lax.broadcasted_iota(jnp.int32, (rows, 128), 1)


def regroup(parts):
    lane = lane_group(parts[0].shape[0])
    step = list(parts)
    bit = len(parts) // 2
    while bit:
        d = 16 * bit
        low = (lane // d) % 2 == 0
        for a in range(len(parts)):
            if a & bit:
                continue
            x, y = step[a], step[a | bit]
            step[a] = jnp.where(low, x, pltpu.roll(y, d, 1))
            step[a | bit] = jnp.where(low, pltpu.roll(x, 128 - d, 1), y)
        bit //= 2
    return step


def column_of(row_ref):
    n = row_ref.shape[1]
    eye = lax.broadcasted_iota(jnp.int32, (n, n), 0) == lax.broadcasted_iota(jnp.int32, (n, n), 1)
    return jnp.sum(jnp.where(eye, row_ref[...], 0.0), axis=1, keepdims=True)


def sums_kernel(x_ref, out_ref):
    x = x_ref[...].astype(F32)
    out_ref[0:1, :] = jnp.sum(x, axis=0, keepdims=True)
    out_ref[1:2, :] = jnp.sum(x * x, axis=0, keepdims=True)


def give_kernel(flags, filter_ref, give_ref, held, ready, sems, out_sems):
    theirs = pl.multiple_of((1 - flags[0]) * HALF, HALF)
    rows = 32
    fetches = []
    for n in range(6):
        part, k = n // 3, n % 3
        fetches.append(
            pltpu.make_async_copy(
                filter_ref.at[part, pl.ds(theirs + rows * k, rows), :], held.at[n], sems.at[n]
            )
        )
        fetches[-1].start()
    sends = []
    for n in range(6):
        part, k = n // 3, n % 3
        fetches[n].wait()
        ready[n] = held[n].astype(BF16)
        sends.append(
            pltpu.make_async_copy(
                ready.at[n], give_ref.at[part, rows * k : rows * (k + 1), :], out_sems.at[n]
            )
        )
        sends[-1].start()
    for send in sends:
        send.wait()


def table_kernel(alpha_ref, beta_ref, w_ref):
    def rows(b, carry):
        start = pl.multiple_of(b * SHARE, SHARE)
        for par in range(2):
            ac = jnp.broadcast_to(alpha_ref[0, pl.ds(b + 32 * par, 1), :], (SHARE, 128))
            as_ = jnp.broadcast_to(alpha_ref[1, pl.ds(b + 32 * par, 1), :], (SHARE, 128))
            for u in range(4 * par, 4 * par + 4):
                bc = beta_ref[0, :, 128 * u : 128 * (u + 1)]
                bs = beta_ref[1, :, 128 * u : 128 * (u + 1)]
                w_ref[pl.ds(start, SHARE), 256 * u : 256 * u + 128] = (ac * bc - as_ * bs).astype(
                    BF16
                )
                w_ref[pl.ds(start, SHARE), 256 * u + 128 : 256 * (u + 1)] = (
                    -(as_ * bc + ac * bs)
                ).astype(BF16)
        return carry

    lax.fori_loop(0, 32, rows, 0)


def forward_kernel(
    x_ref, s0, s1, s2, s3, gain_ref, w_ref, send_ref, normed_ref, kept_ref, fold, sem
):
    keep = pltpu.make_async_copy(w_ref, kept_ref, sem)
    keep.start()
    total = s0[...] + s1[...] + s2[...] + s3[...]
    mean = total[0:1, :] / D
    square = total[1:2, :] / D
    scale = lax.rsqrt(square - mean * mean + 1e-05)
    xn = ((x_ref[...].astype(F32) - mean) * scale * column_of(gain_ref)).astype(BF16)
    normed_ref[...] = xn
    left = xn[:, : TOK // 2].astype(F32)
    right = xn[:, TOK // 2 :].astype(F32)
    fold[0] = (left + right).astype(BF16)
    fold[1] = (left - right).astype(BF16)
    for b in range(4):
        y = [
            jnp.dot(
                fold[par],
                w_ref[:, 1024 * par + 256 * b : 1024 * par + 256 * (b + 1)],
                preferred_element_type=F32,
            )
            for par in range(2)
        ]
        for half in range(2):
            both = []
            for part in range(2):
                both.append(
                    regroup(
                        [
                            y[par][
                                half * HALF + w * QUART : half * HALF + (w + 1) * QUART,
                                128 * part : 128 * (part + 1),
                            ]
                            for par in range(2)
                            for w in range(4)
                        ]
                    )
                )
            for v in range(8):
                q = 8 * b + v
                dest = 63 - q if half else q
                send_ref[dest] = jnp.concatenate([both[0][v], both[1][v]], axis=0).astype(BF16)
    keep.wait()


def lanes_of(rows):
    lane = lax.broadcasted_iota(jnp.int32, (rows, 128), 1)
    group = (lane // 16) % 4
    return 2 * (lane % 16) + lane // 64, group


def make_gains(flags, own_ref, got_ref, ca_ref, cb_ref, g_ref, lhs, prod):
    high = flags[0] == 1
    first = flags[1] == 1
    row = lax.broadcasted_iota(jnp.int32, (128, 128), 0)
    freq, group = lanes_of(128)
    lane = SHARE * group + freq
    straight = jnp.where(row == lane, 1.0, 0.0)
    mirror = jnp.where((row + lane == 128) & (freq != 0), 1.0, 0.0)
    crow = lax.broadcasted_iota(jnp.int32, (NSEQ, 128), 0)
    cfreq, cgroup = lanes_of(NSEQ)
    keep = jnp.where(first, 0.0, 1.0)

    def column(part):
        return (ca_ref[part].astype(F32) + cb_ref[part].astype(F32)).astype(BF16)

    for part in range(2):
        sign = 1.0 if part == 0 else -1.0
        maps = jnp.concatenate([straight, sign * mirror], axis=0).astype(BF16)
        crossed = jnp.concatenate(
            [
                jnp.where((cfreq == 0) & (crow == 63 - 4 * t - cgroup), sign * keep, 0.0)
                for t in range(16)
            ],
            axis=1,
        ).astype(BF16)
        extra = jnp.dot(column(part), crossed, preferred_element_type=F32)
        own = own_ref[part]
        got = got_ref[part]
        direct = jnp.where(high, got, own)
        other = jnp.where(high, own, got)
        for t in range(16):
            rows = slice(HALF * t, HALF * (t + 1))
            lhs[rows, 0:128] = direct[:, 128 * t : 128 * (t + 1)]
            lhs[rows, 128:256] = other[:, 128 * (15 - t) : 128 * (16 - t)]
        prod[...] = jnp.dot(lhs[...], maps, preferred_element_type=F32)
        for t in range(16):
            out = regroup(
                [
                    prod[HALF * t + w * QUART : HALF * t + (w + 1) * QUART, :]
                    + extra[w * QUART : (w + 1) * QUART, 128 * t : 128 * (t + 1)]
                    for w in range(4)
                ]
            )
            for v in range(4):
                g_ref[part, 4 * t + v, 0:QUART, :] = out[v]

    @pl.when(first)
    def _():
        wide = [ca_ref[part].astype(F32) + cb_ref[part].astype(F32) for part in range(2)]
        alone = None
        for k in range(3):
            plain = jnp.concatenate(
                [
                    jnp.where((cfreq == 2 * k) & (crow == 4 * t + cgroup), 1.0, 0.0)
                    for t in range(16)
                ],
                axis=1,
            ).astype(BF16)
            rows = jnp.concatenate(
                [
                    wide[part][w * QUART + 8 * k : w * QUART + 8 * k + 8]
                    for part in range(2)
                    for w in range(4)
                ],
                axis=0,
            ).astype(BF16)
            more = jnp.dot(rows, plain, preferred_element_type=F32)
            alone = more if alone is None else alone + more
        for part in range(2):
            for t in range(16):
                out = regroup(
                    [
                        alone[32 * part + 8 * w : 32 * part + 8 * w + 8, 128 * t : 128 * (t + 1)]
                        for w in range(4)
                    ]
                )
                for v in range(4):
                    g_ref[part, 4 * t + v, QUART:32, :] = out[v]


def packed(tiles):
    return tiles[0] + pltpu.roll(tiles[1], 1, 1) + pltpu.roll(tiles[2], 2, 1)


def turn_i(re, im, s):
    return (-im, re) if s > 0 else (im, -re)


def dft4(xr, xi, s):
    ar, ai = xr[0] + xr[2], xi[0] + xi[2]
    br, bi = xr[0] - xr[2], xi[0] - xi[2]
    cr, ci = xr[1] + xr[3], xi[1] + xi[3]
    dr, di = turn_i(xr[1] - xr[3], xi[1] - xi[3], s)
    return [ar + cr, br + dr, ar - cr, br - dr], [ai + ci, bi + di, ai - ci, bi - di]


def dft8(xr, xi, s):
    er, ei = dft4(xr[0::2], xi[0::2], s)
    dr, di = dft4(xr[1::2], xi[1::2], s)
    c = ROOT_HALF
    if s > 0:
        dr1, di1 = c * (dr[1] - di[1]), c * (di[1] + dr[1])
        dr3, di3 = -c * (dr[3] + di[3]), c * (dr[3] - di[3])
    else:
        dr1, di1 = c * (dr[1] + di[1]), c * (di[1] - dr[1])
        dr3, di3 = c * (di[3] - dr[3]), -c * (di[3] + dr[3])
    dr2, di2 = turn_i(dr[2], di[2], s)
    qr = [dr[0], dr1, dr2, dr3]
    qi = [di[0], di1, di2, di3]
    return (
        [er[k] + qr[k] for k in range(4)] + [er[k] - qr[k] for k in range(4)],
        [ei[k] + qi[k] for k in range(4)] + [ei[k] - qi[k] for k in range(4)],
    )


def twiddle(re, im, index, s):
    index %= 64
    if index == 0:
        return re, im
    c = math.cos(2.0 * math.pi * index / 64.0)
    d = s * math.sin(2.0 * math.pi * index / 64.0)
    return re * c - im * d, im * c + re * d


def across(load, store, gains, a_ref, b_ref):
    for p0 in range(8):
        xr, xi = zip(*[load(p0 + 8 * p1) for p1 in range(8)])
        yr, yi = dft8(list(xr), list(xi), -1)
        for g1 in range(8):
            a_ref[0, g1 * 8 + p0], a_ref[1, g1 * 8 + p0] = twiddle(yr[g1], yi[g1], p0 * g1, -1)
    for g1 in range(8):
        yr, yi = dft8(
            [a_ref[0, g1 * 8 + p0] for p0 in range(8)],
            [a_ref[1, g1 * 8 + p0] for p0 in range(8)],
            -1,
        )
        for g2 in range(8):
            hr, hi = gains(g1 + 8 * g2)
            yr[g2], yi[g2] = hr * yr[g2] - hi * yi[g2], hr * yi[g2] + hi * yr[g2]
        zr, zi = dft8(yr, yi, 1)
        for p0 in range(8):
            b_ref[0, p0 * 8 + g1], b_ref[1, p0 * 8 + g1] = twiddle(zr[p0], zi[p0], g1 * p0, 1)
    for p0 in range(8):
        zr, zi = dft8(
            [b_ref[0, p0 * 8 + g1] for g1 in range(8)],
            [b_ref[1, p0 * 8 + g1] for g1 in range(8)],
            1,
        )
        for p1 in range(8):
            store(p0 + 8 * p1, zr[p1], zi[p1])


def middle_kernel(
    flags, moved, own_ref, got, ca_ref, cb_ref, out_ref,
    moved_ref, got_ref, g_ref, lhs, prod, xr_ref, xi_ref, a_ref, b_ref, sems,
):
    first = flags[1] == 1
    fetches = [
        pltpu.make_async_copy(got, got_ref, sems.at[0]),
        pltpu.make_async_copy(moved, moved_ref, sems.at[1]),
    ]
    for fetch in fetches:
        fetch.start()
    freq, _ = lanes_of(QUART)
    special = (freq == 0) & first
    fetches[0].wait()
    make_gains(flags, own_ref, got_ref, ca_ref, cb_ref, g_ref, lhs, prod)
    fetches[1].wait()

    def widen(p, carry):
        both = moved_ref[p].astype(F32)
        xr_ref[p, 0:QUART, :] = both[:QUART]
        xi_ref[p, 0:QUART, :] = jnp.where(special, 0.0, both[QUART:])
        return carry

    lax.fori_loop(0, NSEQ, widen, 0, unroll=8)

    def half_turn(p):
        return math.cos(2.0 * math.pi * p / 128.0), math.sin(2.0 * math.pi * p / 128.0)

    @pl.when(first)
    def _():
        for p in range(NSEQ):
            c, s = half_turn(p)
            im = jnp.where(special, moved_ref[p].astype(F32)[QUART:], 0.0)
            im = packed([im[8 * k : 8 * k + 8] for k in range(3)])
            xr_ref[p, QUART:32, :] = im * c
            xi_ref[p, QUART:32, :] = im * (-s)

    def every(i, carry):
        rows = pl.ds(pl.multiple_of(i * 8, 8), 8)

        def load(p):
            return xr_ref[p, rows, :], xi_ref[p, rows, :]

        def store(p, re, im):
            xr_ref[p, rows, :] = re
            xi_ref[p, rows, :] = im

        across(load, store, lambda g: (g_ref[0, g, rows, :], g_ref[1, g, rows, :]), a_ref, b_ref)
        return carry

    lax.fori_loop(0, 3 + flags[1], every, 0)

    @pl.when(first)
    def _():
        for p in range(NSEQ):
            c, s = half_turn(p)
            one = xr_ref[p, QUART:32, :] * c - xi_ref[p, QUART:32, :] * s
            alone = jnp.concatenate([one, pltpu.roll(one, 127, 1), pltpu.roll(one, 126, 1)], axis=0)
            xi_ref[p, 0:QUART, :] = jnp.where(special, alone, xi_ref[p, 0:QUART, :])

    def narrow(p, carry):
        out_ref[p] = jnp.concatenate(
            [xr_ref[p, 0:QUART, :], xi_ref[p, 0:QUART, :]], axis=0
        ).astype(BF16)
        return carry

    lax.fori_loop(0, NSEQ, narrow, 0, unroll=8)


def in_three(x):
    a = x.astype(BF16)
    rest = x - a.astype(F32)
    b = rest.astype(BF16)
    return [a, b, (rest - b.astype(F32)).astype(BF16)]


def tokens_back(
    flags, values, w_ref, x_ref, normed_ref, skip, gain, st_in, mix_t_ref, res_ref, outs, tm, st,
    fetches,
    chunk,
):
    me = flags[2]
    skip = skip[...]
    gain = gain[...]
    st[...] = st_in[...]
    for n in range(TC // 512):
        mine = slice(256 * n, 256 * (n + 1))
        fetches[n].wait()
        even, odd = (
            lax.dot_general(
                values[:, 1024 * par : 1024 * (par + 1)],
                w_ref[mine, 1024 * par : 1024 * (par + 1)],
                (((1,), (1,)), ((), ())),
                preferred_element_type=F32,
            )
            for par in range(2)
        )
        for side, conv in enumerate((even + odd, even - odd)):
            here = slice(side * TC // 2 + 256 * n, side * TC // 2 + 256 * (n + 1))
            start = side * TOK // 2 + chunk * TC // 2 + 256 * n
            cols = slice(start, start + 256)
            res = (
                x_ref[:, cols].astype(F32)
                + conv * (1.0 / LENGTH)
                + skip * normed_ref[:, cols].astype(F32)
            ).astype(BF16)
            res_ref[:, here] = res
            r = res.astype(F32)
            mean = jnp.sum(r, axis=0, keepdims=True) * (1.0 / CH)
            centred = r - mean
            for k, part in enumerate(in_three(mean)):
                st[k : k + 1, here] = part.astype(F32)
            for k, part in enumerate(
                in_three(jnp.sum(centred * centred, axis=0, keepdims=True))[:2]
            ):
                st[3 + k : 4 + k, here] = part.astype(F32)
            z = (centred * gain).astype(BF16)
            tm[:, here] = jnp.dot(mix_t_ref[...], z, preferred_element_type=F32)
    for k in range(4):
        rows = pl.ds(pl.multiple_of((me ^ k) * PIECE, PIECE), PIECE)
        outs[k][...] = jnp.concatenate([tm[rows, :], st[...]], axis=0).astype(BF16)


def fetch_table(w_hbm, w_ref, sems, chunk):
    fetches = []
    for n in range(TC // 512):
        here = slice(256 * n, 256 * (n + 1))
        there = slice(chunk * TC // 2 + 256 * n, chunk * TC // 2 + 256 * (n + 1))
        fetches.append(pltpu.make_async_copy(w_hbm.at[there, :], w_ref.at[here, :], sems.at[n]))
        fetches[-1].start()
    return fetches


def back_first_kernel(
    flags, got_ref, w_hbm, x_ref, normed_ref, skip_ref, gain_ref, st_in, mix_t_ref,
    values_ref, res_ref, u0, u1, u2, u3, tall, tm, st, w_ref, sems,
):
    fetches = fetch_table(w_hbm, w_ref, sems, 0)
    for half in range(2):
        for b in range(4):
            parts = []
            for v in range(8):
                q = 8 * b + v
                parts.append(got_ref[63 - q if half else q].astype(F32))
            out = regroup(parts)
            for k in range(8):
                low = half * HALF + (k % 4) * QUART
                left = 1024 * (k // 4) + 256 * b
                tall[low : low + QUART, left : left + 128] = out[k][:QUART]
                tall[low : low + QUART, left + 128 : left + 256] = out[k][QUART:]
    values = tall[...].astype(BF16)
    values_ref[...] = values
    tokens_back(
        flags, values_ref[...], w_ref, x_ref, normed_ref, skip_ref, gain_ref, st_in, mix_t_ref, res_ref,
        (u0, u1, u2, u3), tm, st, fetches, 0,
    )


def back_second_kernel(
    flags, values_ref, w_hbm, x_ref, normed_ref, skip_ref, gain_ref, st_in, mix_t_ref,
    res_ref, u0, u1, u2, u3, tm, st, w_ref, sems,
):
    fetches = fetch_table(w_hbm, w_ref, sems, 1)
    tokens_back(
        flags, values_ref[...], w_ref, x_ref, normed_ref, skip_ref, gain_ref, st_in, mix_t_ref, res_ref,
        (u0, u1, u2, u3), tm, st, fetches, 1,
    )


def mlp_kernel(flags, p0, p1, p2, p3, up_t, down_t, o0, o1, o2, o3, f_ref, low_ref):
    me = flags[2]
    values = [p[...].astype(F32) for p in (p0, p1, p2, p3)]
    tails = [x[PIECE:ROWS] for x in values]
    means = [t[0:1] + t[1:2] + t[2:3] for t in tails]
    mean = (means[0] + means[1] + means[2] + means[3]) * 0.25
    spread = sum(t[3:4] + t[4:5] for t in tails) + CH * sum((m - mean) * (m - mean) for m in means)
    scale = lax.rsqrt(spread * (1.0 / D) + 1e-05)
    row = lax.broadcasted_iota(jnp.int32, (PIECE, CH), 0)
    lane = lax.broadcasted_iota(jnp.int32, (PIECE, CH), 1)
    pick = lane == row + me * PIECE
    for k in range(4):
        line = tails[k][5:6, 0:CH] + tails[k][6:7, 0:CH]
        weight = jnp.sum(jnp.where(pick, line, 0.0), axis=1, keepdims=True)
        f_ref[pl.ds(pl.multiple_of((me ^ k) * PIECE, PIECE), PIECE), :] = scale * (
            values[k][:PIECE] - (mean - means[k]) * weight
        )
    for n in range(TC // 256):
        cols = slice(256 * n, 256 * (n + 1))
        f = f_ref[:, cols].astype(BF16)
        total = None
        for h in range(3):
            rows = slice(256 * h, 256 * (h + 1))
            wide = jnp.dot(up_t[rows, :], f, preferred_element_type=F32)
            act = (0.5 * wide * (1.0 + lax.erf(wide * ROOT_HALF))).astype(BF16)
            part = jnp.dot(down_t[:, rows], act, preferred_element_type=F32)
            total = part if total is None else total + part
        low_ref[:, cols] = total
    for k, o in enumerate((o0, o1, o2, o3)):
        o[...] = low_ref[pl.ds(pl.multiple_of((me ^ k) * PIECE, PIECE), PIECE), :].astype(BF16)


def up_kernel(skip_row, gain_row, mix_in_ref, up_ref, skip_ref, gain_ref, st_ref, in_t, up_t, square, wide):
    skip_ref[...] = column_of(skip_row)
    gain_ref[...] = column_of(gain_row)

    def unroll(src, dst, rows, cols):
        def step(i, carry):
            for k in range(8):
                row = i * 8 + k
                start = pl.multiple_of(row * cols, 128)
                dst[pl.ds(row, 1), :] = src[:, pl.ds(start, cols)].astype(F32)
            return carry

        lax.fori_loop(0, rows // 8, step, 0)

    unroll(up_ref, wide, CH, HID)
    up_t[...] = wide[...].T.astype(BF16)
    paired(mix_in_ref, square, CH)
    in_t[...] = square[...].T.astype(BF16)
    st_ref[...] = jnp.zeros((8, TC), F32)
    weight = jnp.dot(
        gain_row[...], square[...], preferred_element_type=F32, precision=lax.Precision.HIGHEST
    )
    for k, part in enumerate(in_three(weight)[:2]):
        st_ref[5 + k : 6 + k, 0:CH] = part.astype(F32)


def down_kernel(down_ref, mix_out_ref, down_t, out_t, square, tall):
    paired(mix_out_ref, square, CH)
    out_t[...] = square[...].T.astype(BF16)
    paired(down_ref, tall, HID)
    down_t[...] = tall[...].T.astype(BF16)


def paired(src, dst, rows):
    def step(i, carry):
        for k in range(4):
            row = i * 8 + 2 * k
            start = pl.multiple_of(row * CH, 128)
            both = src[:, pl.ds(start, 2 * CH)].astype(F32)
            dst[pl.ds(row, 1), :] = both[:, :CH]
            dst[pl.ds(row + 1, 1), :] = both[:, CH:]
        return carry

    lax.fori_loop(0, rows // 8, step, 0)


def tokens_out(flags, pieces, res_ref, mix_t_ref, f_ref, store):
    me = flags[2]
    for k in range(4):
        rows = pl.ds(pl.multiple_of((me ^ k) * PIECE, PIECE), PIECE)
        f_ref[rows, :] = pieces[k][...].astype(F32)
    for n in range(TC // 256):
        cols = slice(256 * n, 256 * (n + 1))
        add = jnp.dot(mix_t_ref[...], f_ref[:, cols].astype(BF16), preferred_element_type=F32)
        store(cols, (res_ref[:, cols].astype(F32) + add).astype(BF16))


def final_first_kernel(flags, p0, p1, p2, p3, res_ref, mix_t_ref, out_ref, f_ref):
    def store(cols, x):
        out_ref[:, cols] = x

    tokens_out(flags, (p0, p1, p2, p3), res_ref, mix_t_ref, f_ref, store)


def final_second_kernel(flags, p0, p1, p2, p3, res_ref, mix_t_ref, early_ref, out_ref, f_ref):
    side = TC // 2
    for k in range(2):
        out_ref[:, 2 * k * side : (2 * k + 1) * side] = early_ref[:, k * side : (k + 1) * side]

    def store(cols, x):
        start = cols.start + (side if cols.start < side else 2 * side)
        out_ref[:, start : start + 256] = x

    tokens_out(flags, (p0, p1, p2, p3), res_ref, mix_t_ref, f_ref, store)


def swap(x, k):
    return lax.ppermute(x, "chan", [(i, i ^ k) for i in range(4)])


def shards(
    tokens, filter_spectrum, skip_weight, norm_gain, mlp_gain, mix_in, up_weight, down_weight, mix_out
):
    return block(
        tokens, filter_spectrum, skip_weight[None], norm_gain[None], mlp_gain[None], mix_in,
        up_weight, down_weight, mix_out,
    )


def block(
    tokens, filter_spectrum, skip_weight, norm_gain, mlp_gain, mix_in, up_weight, down_weight, mix_out
):
    place = lax.axis_index("seq")
    lane_of = lax.axis_index("chan")
    high = place >= 32
    first = (place == 0) | (place == 63)
    flags = jnp.stack([high, first, lane_of, place]).astype(jnp.int32)
    mine = jnp.where(high, HALF, 0)
    give = call(
        give_kernel, pltpu.HBM((2, HALF, TOK), BF16), "sh",
        scratch=[
            pltpu.VMEM((6, 32, TOK), F32), pltpu.VMEM((6, 32, TOK), BF16),
            pltpu.SemaphoreType.DMA((6,)), pltpu.SemaphoreType.DMA((6,)),
        ],
        outs="h",
    )(flags, in_hbm(filter_spectrum))
    got = lax.ppermute(give, "seq", [(i, 63 - i) for i in range(64)])
    sums = call(sums_kernel, shape((2, TOK), F32), "v")(tokens)
    others = []
    for k in (1, 2, 3):
        others.append(swap(sums, k))
    own = lax.dynamic_slice_in_dim(filter_spectrum, mine, HALF, 1).astype(BF16)
    pick_row = jnp.arange(TOK, dtype=jnp.int32)[:, None]
    pick_col = jnp.arange(NSEQ, dtype=jnp.int32)[None, :]
    pick = (pick_row == SHARE * pick_col).astype(BF16)
    column = jnp.einsum(
        "pcj,jg->pcg", filter_spectrum.astype(BF16), pick, preferred_element_type=F32
    ).astype(BF16)
    ca = lax.ppermute(column[:, :HALF], "seq", [(32, 0)] + [(64 - i, i) for i in range(1, 32)])
    cb = lax.ppermute(column[:, HALF:], "seq", [(32, 63)] + [(i + 1, i) for i in range(32, 63)])
    slot = jnp.arange(TOK // 2, dtype=jnp.int32)
    freq = 256 * (slot // 128 % 4) + 2 * (slot % 128) + slot // 512
    step = jnp.arange(SHARE, dtype=jnp.int32)
    angle = (freq[None, :] * (64 * step[:, None] + place) % LENGTH).astype(F32) * (
        2.0 * math.pi / LENGTH
    )
    parity = 1.0 - 2.0 * (step % 2).astype(F32)
    beta = jnp.stack(
        [jnp.cos(angle), jnp.where(freq[None, :] == 0, -parity[:, None], jnp.sin(angle))]
    )
    half_row = jnp.arange(64, dtype=jnp.int32)[:, None]
    half_freq = 2 * jnp.arange(128, dtype=jnp.int32)[None, :] + half_row // 32
    turn = ((half_row % 32) * half_freq % 64).astype(F32) * (2.0 * math.pi / 64)
    alpha = jnp.stack([jnp.cos(turn), jnp.sin(turn)])
    table = call(table_kernel, shape((TOK // 2, TOK), BF16), "vv")(alpha, beta)
    send, normed, kept = call(
        forward_kernel,
        (
            shape((NSEQ, 2 * QUART, 128), BF16),
            shape((CH, TOK), BF16),
            pltpu.HBM((TOK // 2, TOK), BF16),
        ),
        "v" * 7,
        scratch=[pltpu.VMEM((2, CH, TOK // 2), BF16), pltpu.SemaphoreType.DMA(())],
        outs="vvh",
        mib=20,
    )(tokens, sums, *others, norm_gain, table)
    moved = lax.all_to_all(send, "seq", split_axis=0, concat_axis=0, tiled=True)
    skip_col, gain_col, st_in, mix_in_t, up_t = call(
        up_kernel,
        (
            shape((CH, 1), F32), shape((CH, 1), F32), shape((8, TC), F32), shape((CH, CH), BF16),
            shape((HID, CH), BF16),
        ),
        "vvvv",
        scratch=[pltpu.VMEM((CH, CH), F32), pltpu.VMEM((CH, HID), F32)],
    )(skip_weight, mlp_gain, mix_in, up_weight)
    moved, skip_col, gain_col, st_in, mix_in_t, up_t = lax.optimization_barrier(
        (moved, skip_col, gain_col, st_in, mix_in_t, up_t)
    )
    back = call(
        middle_kernel,
        shape((NSEQ, 2 * QUART, 128), BF16),
        "shvhvv",
        scratch=[
            pltpu.VMEM((NSEQ, 2 * QUART, 128), BF16),
            pltpu.VMEM((2, HALF, TOK), BF16),
            pltpu.VMEM((2, NSEQ, 32, 128), F32),
            pltpu.VMEM((16 * HALF, 256), BF16),
            pltpu.VMEM((16 * HALF, 128), F32),
            pltpu.VMEM((NSEQ, 32, 128), F32),
            pltpu.VMEM((NSEQ, 32, 128), F32),
            pltpu.VMEM((2, NSEQ, 8, 128), F32),
            pltpu.VMEM((2, NSEQ, 8, 128), F32),
            pltpu.SemaphoreType.DMA((2,)),
        ],
    )(flags, in_hbm(moved), own, in_hbm(got), ca, cb)
    back, down_weight, mix_out = lax.optimization_barrier((back, down_weight, mix_out))
    down_t, mix_out_t = call(
        down_kernel,
        (shape((CH, HID), BF16), shape((CH, CH), BF16)),
        "vv",
        scratch=[pltpu.VMEM((CH, CH), F32), pltpu.VMEM((HID, CH), F32)],
    )(down_weight, mix_out)
    home = lax.all_to_all(back, "seq", split_axis=0, concat_axis=0, tiled=True)
    home, down_t, mix_out_t = lax.optimization_barrier((home, down_t, mix_out_t))
    piece = (shape((CH, TC), BF16),) + (shape((ROWS, TC), BF16),) * 4
    small = [
        pltpu.VMEM((CH, TC), F32),
        pltpu.VMEM((8, TC), F32),
        pltpu.VMEM((TC // 2, TOK), BF16),
        pltpu.SemaphoreType.DMA((TC // 512,)),
    ]
    rest = (in_hbm(kept), tokens, normed, skip_col, gain_col, st_in, mix_in_t)
    values, res_a, *first_a = call(
        back_first_kernel, (shape((CH, TOK), BF16),) + piece, "svhvvvvvv",
        scratch=[pltpu.VMEM((CH, TOK), F32)] + small, mib=20,
    )(flags, home, *rest)
    arrived_a = [first_a[0]] + [swap(first_a[k], k) for k in (1, 2, 3)]
    res_b, *first_b = call(
        back_second_kernel, piece, "svhvvvvvv", scratch=small, mib=20
    )(flags, values, *rest)
    arrived_b = [first_b[0]] + [swap(first_b[k], k) for k in (1, 2, 3)]

    def mlp(arrived):
        lows = call(
            mlp_kernel,
            (shape((PIECE, TC), BF16),) * 4,
            "s" + "v" * 6,
            scratch=[pltpu.VMEM((CH, TC), F32), pltpu.VMEM((CH, TC), F32)],
        )(flags, *arrived, up_t, down_t)
        return [lows[0]] + [swap(lows[k], k) for k in (1, 2, 3)]

    back_home_a = mlp(arrived_a)
    back_home_b = mlp(arrived_b)
    early = call(
        final_first_kernel, shape((CH, TC), BF16), "s" + "v" * 6, scratch=[pltpu.VMEM((CH, TC), F32)],
    )(flags, *back_home_a, res_a, mix_out_t)
    return call(
        final_second_kernel, shape((CH, TOK), BF16), "s" + "v" * 7, scratch=[pltpu.VMEM((CH, TC), F32)],
    )(flags, *back_home_b, res_b, mix_out_t, early)


def solution(mesh):
    in_specs = (
        P("chan", "seq"),
        P(None, "chan", "seq"),
        P("chan"),
        P("chan"),
        P("chan"),
        P("chan", None),
        P("chan", None),
        P("chan", None),
        P("chan", None),
    )
    out_specs = P("chan", "seq")
    return jax.shard_map(shards, mesh=mesh, in_specs=in_specs, out_specs=out_specs, check_vma=False)
```

```python
import math

import jax
import jax.numpy as jnp
from jax import lax
from jax.experimental import pallas as pl
from jax.experimental.pallas import tpu as pltpu
from jax.sharding import PartitionSpec as P


D = 768
CH = 192
HALF = 96
QUART = 24
TOK = 2048
NSEQ = 64
SHARE = 32
LENGTH = TOK * NSEQ
HID = 768
PIECE = 48
CHUNKS = 2
TC = TOK // CHUNKS
F32 = jnp.float32
BF16 = jnp.bfloat16
ROOT_HALF = math.sqrt(0.5)
MIB = 1024 * 1024
ROWS = 56


def vm():
    return pl.BlockSpec(memory_space=pltpu.VMEM)


def sm():
    return pl.BlockSpec(memory_space=pltpu.SMEM)


def hb():
    return pl.BlockSpec(memory_space=pltpu.HBM)


def call(body, out_shape, kinds, scratch=(), mib=14, outs=None):
    spec = {"s": sm, "v": vm, "h": hb}
    many = isinstance(out_shape, (tuple, list))
    outs = outs or "v" * (len(out_shape) if many else 1)
    return pl.pallas_call(
        body,
        out_shape=out_shape,
        in_specs=[spec[k]() for k in kinds],
        out_specs=[spec[k]() for k in outs] if many else spec[outs](),
        scratch_shapes=scratch,
        compiler_params=pltpu.CompilerParams(vmem_limit_bytes=mib * MIB),
    )


def in_hbm(x):
    return pltpu.with_memory_space_constraint(x, pltpu.HBM)


def shape(dims, dtype):
    return jax.ShapeDtypeStruct(dims, dtype)


def lane_group(rows):
    return lax.broadcasted_iota(jnp.int32, (rows, 128), 1)


def regroup(parts):
    lane = lane_group(parts[0].shape[0])
    step = list(parts)
    bit = len(parts) // 2
    while bit:
        d = 16 * bit
        low = (lane // d) % 2 == 0
        for a in range(len(parts)):
            if a & bit:
                continue
            x, y = step[a], step[a | bit]
            step[a] = jnp.where(low, x, pltpu.roll(y, d, 1))
            step[a | bit] = jnp.where(low, pltpu.roll(x, 128 - d, 1), y)
        bit //= 2
    return step


def column_of(row_ref):
    n = row_ref.shape[1]
    eye = lax.broadcasted_iota(jnp.int32, (n, n), 0) == lax.broadcasted_iota(jnp.int32, (n, n), 1)
    return jnp.sum(jnp.where(eye, row_ref[...], 0.0), axis=1, keepdims=True)


def sums_kernel(x_ref, out_ref):
    x = x_ref[...].astype(F32)
    out_ref[0:1, :] = jnp.sum(x, axis=0, keepdims=True)
    out_ref[1:2, :] = jnp.sum(x * x, axis=0, keepdims=True)


def give_kernel(flags, filter_ref, give_ref, held, sems):
    theirs = pl.multiple_of((1 - flags[0]) * HALF, HALF)
    rows = 32
    fetches = []
    for n in range(6):
        part, k = n // 3, n % 3
        fetches.append(
            pltpu.make_async_copy(
                filter_ref.at[part, pl.ds(theirs + rows * k, rows), :], held.at[n], sems.at[n]
            )
        )
        fetches[-1].start()
    for n in range(6):
        part, k = n // 3, n % 3
        fetches[n].wait()
        give_ref[part, rows * k : rows * (k + 1), :] = held[n].astype(BF16)


def table_kernel(alpha_ref, beta_ref, w_ref):
    def rows(b, carry):
        start = pl.multiple_of(b * SHARE, SHARE)
        for par in range(2):
            ac = jnp.broadcast_to(alpha_ref[0, pl.ds(b + 32 * par, 1), :], (SHARE, 128))
            as_ = jnp.broadcast_to(alpha_ref[1, pl.ds(b + 32 * par, 1), :], (SHARE, 128))
            for u in range(4 * par, 4 * par + 4):
                bc = beta_ref[0, :, 128 * u : 128 * (u + 1)]
                bs = beta_ref[1, :, 128 * u : 128 * (u + 1)]
                w_ref[pl.ds(start, SHARE), 256 * u : 256 * u + 128] = (ac * bc - as_ * bs).astype(
                    BF16
                )
                w_ref[pl.ds(start, SHARE), 256 * u + 128 : 256 * (u + 1)] = (
                    -(as_ * bc + ac * bs)
                ).astype(BF16)
        return carry

    lax.fori_loop(0, 32, rows, 0)


def forward_kernel(
    x_ref, s0, s1, s2, s3, gain_ref, w_ref, send_ref, normed_ref, kept_ref, fold, sem
):
    keep = pltpu.make_async_copy(w_ref, kept_ref, sem)
    keep.start()
    total = s0[...] + s1[...] + s2[...] + s3[...]
    mean = total[0:1, :] / D
    square = total[1:2, :] / D
    scale = lax.rsqrt(square - mean * mean + 1e-05)
    xn = ((x_ref[...].astype(F32) - mean) * scale * column_of(gain_ref)).astype(BF16)
    normed_ref[...] = xn
    left = xn[:, : TOK // 2].astype(F32)
    right = xn[:, TOK // 2 :].astype(F32)
    fold[0] = (left + right).astype(BF16)
    fold[1] = (left - right).astype(BF16)
    for b in range(4):
        y = [
            jnp.dot(
                fold[par],
                w_ref[:, 1024 * par + 256 * b : 1024 * par + 256 * (b + 1)],
                preferred_element_type=F32,
            )
            for par in range(2)
        ]
        for half in range(2):
            both = []
            for part in range(2):
                both.append(
                    regroup(
                        [
                            y[par][
                                half * HALF + w * QUART : half * HALF + (w + 1) * QUART,
                                128 * part : 128 * (part + 1),
                            ]
                            for par in range(2)
                            for w in range(4)
                        ]
                    )
                )
            for v in range(8):
                q = 8 * b + v
                dest = 63 - q if half else q
                send_ref[dest] = jnp.concatenate([both[0][v], both[1][v]], axis=0).astype(BF16)
    keep.wait()


def lanes_of(rows):
    lane = lax.broadcasted_iota(jnp.int32, (rows, 128), 1)
    group = (lane // 16) % 4
    return 2 * (lane % 16) + lane // 64, group


def make_gains(flags, own_ref, got_ref, ca_ref, cb_ref, g_ref, lhs, prod):
    high = flags[0] == 1
    first = flags[1] == 1
    row = lax.broadcasted_iota(jnp.int32, (128, 128), 0)
    freq, group = lanes_of(128)
    lane = SHARE * group + freq
    straight = jnp.where(row == lane, 1.0, 0.0)
    mirror = jnp.where((row + lane == 128) & (freq != 0), 1.0, 0.0)
    crow = lax.broadcasted_iota(jnp.int32, (NSEQ, 128), 0)
    cfreq, cgroup = lanes_of(NSEQ)
    keep = jnp.where(first, 0.0, 1.0)

    def column(part):
        return (ca_ref[part].astype(F32) + cb_ref[part].astype(F32)).astype(BF16)

    for part in range(2):
        sign = 1.0 if part == 0 else -1.0
        maps = jnp.concatenate([straight, sign * mirror], axis=0).astype(BF16)
        crossed = jnp.concatenate(
            [
                jnp.where((cfreq == 0) & (crow == 63 - 4 * t - cgroup), sign * keep, 0.0)
                for t in range(16)
            ],
            axis=1,
        ).astype(BF16)
        extra = jnp.dot(column(part), crossed, preferred_element_type=F32)
        own = own_ref[part]
        got = got_ref[part]
        direct = jnp.where(high, got, own)
        other = jnp.where(high, own, got)
        for t in range(16):
            rows = slice(HALF * t, HALF * (t + 1))
            lhs[rows, 0:128] = direct[:, 128 * t : 128 * (t + 1)]
            lhs[rows, 128:256] = other[:, 128 * (15 - t) : 128 * (16 - t)]
        prod[...] = jnp.dot(lhs[...], maps, preferred_element_type=F32)
        for t in range(16):
            out = regroup(
                [
                    prod[HALF * t + w * QUART : HALF * t + (w + 1) * QUART, :]
                    + extra[w * QUART : (w + 1) * QUART, 128 * t : 128 * (t + 1)]
                    for w in range(4)
                ]
            )
            for v in range(4):
                g_ref[part, 4 * t + v, 0:QUART, :] = out[v]

    @pl.when(first)
    def _():
        wide = [ca_ref[part].astype(F32) + cb_ref[part].astype(F32) for part in range(2)]
        alone = None
        for k in range(3):
            plain = jnp.concatenate(
                [
                    jnp.where((cfreq == 2 * k) & (crow == 4 * t + cgroup), 1.0, 0.0)
                    for t in range(16)
                ],
                axis=1,
            ).astype(BF16)
            rows = jnp.concatenate(
                [
                    wide[part][w * QUART + 8 * k : w * QUART + 8 * k + 8]
                    for part in range(2)
                    for w in range(4)
                ],
                axis=0,
            ).astype(BF16)
            more = jnp.dot(rows, plain, preferred_element_type=F32)
            alone = more if alone is None else alone + more
        for part in range(2):
            for t in range(16):
                out = regroup(
                    [
                        alone[32 * part + 8 * w : 32 * part + 8 * w + 8, 128 * t : 128 * (t + 1)]
                        for w in range(4)
                    ]
                )
                for v in range(4):
                    g_ref[part, 4 * t + v, QUART:32, :] = out[v]


def packed(tiles):
    return tiles[0] + pltpu.roll(tiles[1], 1, 1) + pltpu.roll(tiles[2], 2, 1)


def turn_i(re, im, s):
    return (-im, re) if s > 0 else (im, -re)


def dft4(xr, xi, s):
    ar, ai = xr[0] + xr[2], xi[0] + xi[2]
    br, bi = xr[0] - xr[2], xi[0] - xi[2]
    cr, ci = xr[1] + xr[3], xi[1] + xi[3]
    dr, di = turn_i(xr[1] - xr[3], xi[1] - xi[3], s)
    return [ar + cr, br + dr, ar - cr, br - dr], [ai + ci, bi + di, ai - ci, bi - di]


def dft8(xr, xi, s):
    er, ei = dft4(xr[0::2], xi[0::2], s)
    dr, di = dft4(xr[1::2], xi[1::2], s)
    c = ROOT_HALF
    if s > 0:
        dr1, di1 = c * (dr[1] - di[1]), c * (di[1] + dr[1])
        dr3, di3 = -c * (dr[3] + di[3]), c * (dr[3] - di[3])
    else:
        dr1, di1 = c * (dr[1] + di[1]), c * (di[1] - dr[1])
        dr3, di3 = c * (di[3] - dr[3]), -c * (di[3] + dr[3])
    dr2, di2 = turn_i(dr[2], di[2], s)
    qr = [dr[0], dr1, dr2, dr3]
    qi = [di[0], di1, di2, di3]
    return (
        [er[k] + qr[k] for k in range(4)] + [er[k] - qr[k] for k in range(4)],
        [ei[k] + qi[k] for k in range(4)] + [ei[k] - qi[k] for k in range(4)],
    )


def twiddle(re, im, index, s):
    index %= 64
    if index == 0:
        return re, im
    c = math.cos(2.0 * math.pi * index / 64.0)
    d = s * math.sin(2.0 * math.pi * index / 64.0)
    return re * c - im * d, im * c + re * d


def across(load, store, gains, a_ref, b_ref):
    for p0 in range(8):
        xr, xi = zip(*[load(p0 + 8 * p1) for p1 in range(8)])
        yr, yi = dft8(list(xr), list(xi), -1)
        for g1 in range(8):
            a_ref[0, g1 * 8 + p0], a_ref[1, g1 * 8 + p0] = twiddle(yr[g1], yi[g1], p0 * g1, -1)
    for g1 in range(8):
        yr, yi = dft8(
            [a_ref[0, g1 * 8 + p0] for p0 in range(8)],
            [a_ref[1, g1 * 8 + p0] for p0 in range(8)],
            -1,
        )
        for g2 in range(8):
            hr, hi = gains(g1 + 8 * g2)
            yr[g2], yi[g2] = hr * yr[g2] - hi * yi[g2], hr * yi[g2] + hi * yr[g2]
        zr, zi = dft8(yr, yi, 1)
        for p0 in range(8):
            b_ref[0, p0 * 8 + g1], b_ref[1, p0 * 8 + g1] = twiddle(zr[p0], zi[p0], g1 * p0, 1)
    for p0 in range(8):
        zr, zi = dft8(
            [b_ref[0, p0 * 8 + g1] for g1 in range(8)],
            [b_ref[1, p0 * 8 + g1] for g1 in range(8)],
            1,
        )
        for p1 in range(8):
            store(p0 + 8 * p1, zr[p1], zi[p1])


def middle_kernel(
    flags, moved, own_ref, got, ca_ref, cb_ref, out_ref,
    moved_ref, got_ref, g_ref, lhs, prod, xr_ref, xi_ref, a_ref, b_ref, sems,
):
    first = flags[1] == 1
    fetches = [
        pltpu.make_async_copy(got, got_ref, sems.at[0]),
        pltpu.make_async_copy(moved, moved_ref, sems.at[1]),
    ]
    for fetch in fetches:
        fetch.start()
    freq, _ = lanes_of(QUART)
    special = (freq == 0) & first
    fetches[0].wait()
    make_gains(flags, own_ref, got_ref, ca_ref, cb_ref, g_ref, lhs, prod)
    fetches[1].wait()

    def widen(p, carry):
        both = moved_ref[p].astype(F32)
        xr_ref[p, 0:QUART, :] = both[:QUART]
        xi_ref[p, 0:QUART, :] = jnp.where(special, 0.0, both[QUART:])
        return carry

    lax.fori_loop(0, NSEQ, widen, 0, unroll=8)

    def half_turn(p):
        return math.cos(2.0 * math.pi * p / 128.0), math.sin(2.0 * math.pi * p / 128.0)

    @pl.when(first)
    def _():
        for p in range(NSEQ):
            c, s = half_turn(p)
            im = jnp.where(special, moved_ref[p].astype(F32)[QUART:], 0.0)
            im = packed([im[8 * k : 8 * k + 8] for k in range(3)])
            xr_ref[p, QUART:32, :] = im * c
            xi_ref[p, QUART:32, :] = im * (-s)

    def every(i, carry):
        rows = pl.ds(pl.multiple_of(i * 8, 8), 8)

        def load(p):
            return xr_ref[p, rows, :], xi_ref[p, rows, :]

        def store(p, re, im):
            xr_ref[p, rows, :] = re
            xi_ref[p, rows, :] = im

        across(load, store, lambda g: (g_ref[0, g, rows, :], g_ref[1, g, rows, :]), a_ref, b_ref)
        return carry

    lax.fori_loop(0, 3 + flags[1], every, 0)

    @pl.when(first)
    def _():
        for p in range(NSEQ):
            c, s = half_turn(p)
            one = xr_ref[p, QUART:32, :] * c - xi_ref[p, QUART:32, :] * s
            alone = jnp.concatenate([one, pltpu.roll(one, 127, 1), pltpu.roll(one, 126, 1)], axis=0)
            xi_ref[p, 0:QUART, :] = jnp.where(special, alone, xi_ref[p, 0:QUART, :])

    def narrow(p, carry):
        out_ref[p] = jnp.concatenate(
            [xr_ref[p, 0:QUART, :], xi_ref[p, 0:QUART, :]], axis=0
        ).astype(BF16)
        return carry

    lax.fori_loop(0, NSEQ, narrow, 0, unroll=8)


def in_three(x):
    a = x.astype(BF16)
    rest = x - a.astype(F32)
    b = rest.astype(BF16)
    return [a, b, (rest - b.astype(F32)).astype(BF16)]


def tokens_back(
    flags, values, w_ref, x_ref, normed_ref, skip, gain, st_in, mix_t_ref, res_ref, outs, tm, st,
    fetches,
    chunk,
):
    me = flags[2]
    skip = skip[...]
    gain = gain[...]
    st[...] = st_in[...]
    for n in range(TC // 512):
        mine = slice(256 * n, 256 * (n + 1))
        sums = []
        for par in range(2):
            fetches[2 * n + par].wait()
            sums.append(
                lax.dot_general(
                    values[:, 1024 * par : 1024 * (par + 1)],
                    w_ref[mine, 1024 * par : 1024 * (par + 1)],
                    (((1,), (1,)), ((), ())),
                    preferred_element_type=F32,
                )
            )
        even, odd = sums
        for side, conv in enumerate((even + odd, even - odd)):
            here = slice(side * TC // 2 + 256 * n, side * TC // 2 + 256 * (n + 1))
            start = side * TOK // 2 + chunk * TC // 2 + 256 * n
            cols = slice(start, start + 256)
            res = (
                x_ref[:, cols].astype(F32)
                + conv * (1.0 / LENGTH)
                + skip * normed_ref[:, cols].astype(F32)
            ).astype(BF16)
            res_ref[:, here] = res
            r = res.astype(F32)
            mean = jnp.sum(r, axis=0, keepdims=True) * (1.0 / CH)
            centred = r - mean
            for k, part in enumerate(in_three(mean)):
                st[k : k + 1, here] = part.astype(F32)
            for k, part in enumerate(
                in_three(jnp.sum(centred * centred, axis=0, keepdims=True))[:2]
            ):
                st[3 + k : 4 + k, here] = part.astype(F32)
            z = (centred * gain).astype(BF16)
            tm[:, here] = jnp.dot(mix_t_ref[...], z, preferred_element_type=F32)
    for k in range(4):
        rows = pl.ds(pl.multiple_of((me ^ k) * PIECE, PIECE), PIECE)
        outs[k][...] = jnp.concatenate([tm[rows, :], st[...]], axis=0).astype(BF16)


def fetch_table(w_hbm, w_ref, sems, chunk):
    fetches = []
    for n in range(TC // 512):
        here = slice(256 * n, 256 * (n + 1))
        there = slice(chunk * TC // 2 + 256 * n, chunk * TC // 2 + 256 * (n + 1))
        for par in range(2):
            cols = slice(1024 * par, 1024 * (par + 1))
            fetches.append(
                pltpu.make_async_copy(
                    w_hbm.at[there, cols], w_ref.at[here, cols], sems.at[2 * n + par]
                )
            )
            fetches[-1].start()
    return fetches


def back_first_kernel(
    flags, got_ref, w_hbm, x_ref, normed_ref, skip_ref, gain_ref, st_in, mix_t_ref,
    values_ref, res_ref, u0, u1, u2, u3, tall, tm, st, w_ref, sems,
):
    fetches = fetch_table(w_hbm, w_ref, sems, 0)
    for half in range(2):
        for b in range(4):
            parts = []
            for v in range(8):
                q = 8 * b + v
                parts.append(got_ref[63 - q if half else q].astype(F32))
            out = regroup(parts)
            for k in range(8):
                low = half * HALF + (k % 4) * QUART
                left = 1024 * (k // 4) + 256 * b
                tall[low : low + QUART, left : left + 128] = out[k][:QUART]
                tall[low : low + QUART, left + 128 : left + 256] = out[k][QUART:]
    values = tall[...].astype(BF16)
    values_ref[...] = values
    tokens_back(
        flags, values_ref[...], w_ref, x_ref, normed_ref, skip_ref, gain_ref, st_in, mix_t_ref, res_ref,
        (u0, u1, u2, u3), tm, st, fetches, 0,
    )


def back_second_kernel(
    flags, values_ref, w_hbm, x_ref, normed_ref, skip_ref, gain_ref, st_in, mix_t_ref,
    res_ref, u0, u1, u2, u3, tm, st, w_ref, sems,
):
    fetches = fetch_table(w_hbm, w_ref, sems, 1)
    tokens_back(
        flags, values_ref[...], w_ref, x_ref, normed_ref, skip_ref, gain_ref, st_in, mix_t_ref, res_ref,
        (u0, u1, u2, u3), tm, st, fetches, 1,
    )


def mlp_kernel(flags, p0, p1, p2, p3, up_t, down_t, o0, o1, o2, o3, f_ref, low_ref):
    me = flags[2]
    values = [p[...].astype(F32) for p in (p0, p1, p2, p3)]
    tails = [x[PIECE:ROWS] for x in values]
    means = [t[0:1] + t[1:2] + t[2:3] for t in tails]
    mean = (means[0] + means[1] + means[2] + means[3]) * 0.25
    spread = sum(t[3:4] + t[4:5] for t in tails) + CH * sum((m - mean) * (m - mean) for m in means)
    scale = lax.rsqrt(spread * (1.0 / D) + 1e-05)
    row = lax.broadcasted_iota(jnp.int32, (PIECE, CH), 0)
    lane = lax.broadcasted_iota(jnp.int32, (PIECE, CH), 1)
    pick = lane == row + me * PIECE
    for k in range(4):
        line = tails[k][5:6, 0:CH] + tails[k][6:7, 0:CH]
        weight = jnp.sum(jnp.where(pick, line, 0.0), axis=1, keepdims=True)
        f_ref[pl.ds(pl.multiple_of((me ^ k) * PIECE, PIECE), PIECE), :] = scale * (
            values[k][:PIECE] - (mean - means[k]) * weight
        )
    for n in range(TC // 256):
        cols = slice(256 * n, 256 * (n + 1))
        f = f_ref[:, cols].astype(BF16)
        total = None
        for h in range(3):
            rows = slice(256 * h, 256 * (h + 1))
            wide = jnp.dot(up_t[rows, :], f, preferred_element_type=F32)
            act = (0.5 * wide * (1.0 + lax.erf(wide * ROOT_HALF))).astype(BF16)
            part = jnp.dot(down_t[:, rows], act, preferred_element_type=F32)
            total = part if total is None else total + part
        low_ref[:, cols] = total
    for k, o in enumerate((o0, o1, o2, o3)):
        o[...] = low_ref[pl.ds(pl.multiple_of((me ^ k) * PIECE, PIECE), PIECE), :].astype(BF16)


def up_kernel(skip_row, gain_row, mix_in_ref, up_ref, skip_ref, gain_ref, st_ref, in_t, up_t, square, wide):
    skip_ref[...] = column_of(skip_row)
    gain_ref[...] = column_of(gain_row)

    def unroll(src, dst, rows, cols):
        def step(i, carry):
            for k in range(8):
                row = i * 8 + k
                start = pl.multiple_of(row * cols, 128)
                dst[pl.ds(row, 1), :] = src[:, pl.ds(start, cols)].astype(F32)
            return carry

        lax.fori_loop(0, rows // 8, step, 0)

    unroll(up_ref, wide, CH, HID)
    up_t[...] = wide[...].T.astype(BF16)
    paired(mix_in_ref, square, CH)
    in_t[...] = square[...].T.astype(BF16)
    st_ref[...] = jnp.zeros((8, TC), F32)
    weight = jnp.dot(
        gain_row[...], square[...], preferred_element_type=F32, precision=lax.Precision.HIGHEST
    )
    for k, part in enumerate(in_three(weight)[:2]):
        st_ref[5 + k : 6 + k, 0:CH] = part.astype(F32)


def down_kernel(down_ref, mix_out_ref, down_t, out_t, square, tall):
    paired(mix_out_ref, square, CH)
    out_t[...] = square[...].T.astype(BF16)
    paired(down_ref, tall, HID)
    down_t[...] = tall[...].T.astype(BF16)


def paired(src, dst, rows):
    def step(i, carry):
        for k in range(4):
            row = i * 8 + 2 * k
            start = pl.multiple_of(row * CH, 128)
            both = src[:, pl.ds(start, 2 * CH)].astype(F32)
            dst[pl.ds(row, 1), :] = both[:, :CH]
            dst[pl.ds(row + 1, 1), :] = both[:, CH:]
        return carry

    lax.fori_loop(0, rows // 8, step, 0)


def tokens_out(flags, pieces, res_ref, mix_t_ref, f_ref, store):
    me = flags[2]
    for k in range(4):
        rows = pl.ds(pl.multiple_of((me ^ k) * PIECE, PIECE), PIECE)
        f_ref[rows, :] = pieces[k][...].astype(F32)
    for n in range(TC // 256):
        cols = slice(256 * n, 256 * (n + 1))
        add = jnp.dot(mix_t_ref[...], f_ref[:, cols].astype(BF16), preferred_element_type=F32)
        store(cols, (res_ref[:, cols].astype(F32) + add).astype(BF16))


def final_first_kernel(flags, p0, p1, p2, p3, res_ref, mix_t_ref, out_ref, f_ref):
    def store(cols, x):
        out_ref[:, cols] = x

    tokens_out(flags, (p0, p1, p2, p3), res_ref, mix_t_ref, f_ref, store)


def final_second_kernel(flags, p0, p1, p2, p3, res_ref, mix_t_ref, early_ref, out_ref, f_ref):
    side = TC // 2
    for k in range(2):
        out_ref[:, 2 * k * side : (2 * k + 1) * side] = early_ref[:, k * side : (k + 1) * side]

    def store(cols, x):
        start = cols.start + (side if cols.start < side else 2 * side)
        out_ref[:, start : start + 256] = x

    tokens_out(flags, (p0, p1, p2, p3), res_ref, mix_t_ref, f_ref, store)


def swap(x, k):
    return lax.ppermute(x, "chan", [(i, i ^ k) for i in range(4)])


def shards(
    tokens, filter_spectrum, skip_weight, norm_gain, mlp_gain, mix_in, up_weight, down_weight, mix_out
):
    return block(
        tokens, filter_spectrum, skip_weight[None], norm_gain[None], mlp_gain[None], mix_in,
        up_weight, down_weight, mix_out,
    )


def block(
    tokens, filter_spectrum, skip_weight, norm_gain, mlp_gain, mix_in, up_weight, down_weight, mix_out
):
    place = lax.axis_index("seq")
    lane_of = lax.axis_index("chan")
    high = place >= 32
    first = (place == 0) | (place == 63)
    flags = jnp.stack([high, first, lane_of, place]).astype(jnp.int32)
    mine = jnp.where(high, HALF, 0)
    give = call(
        give_kernel, shape((2, HALF, TOK), BF16), "sh",
        scratch=[pltpu.VMEM((6, 32, TOK), F32), pltpu.SemaphoreType.DMA((6,))],
    )(flags, in_hbm(filter_spectrum))
    got = lax.ppermute(give, "seq", [(i, 63 - i) for i in range(64)])
    sums = call(sums_kernel, shape((2, TOK), F32), "v")(tokens)
    others = []
    for k in (1, 2, 3):
        others.append(swap(sums, k))
    own = lax.dynamic_slice_in_dim(filter_spectrum, mine, HALF, 1).astype(BF16)
    pick_row = jnp.arange(TOK, dtype=jnp.int32)[:, None]
    pick_col = jnp.arange(NSEQ, dtype=jnp.int32)[None, :]
    pick = (pick_row == SHARE * pick_col).astype(BF16)
    column = jnp.einsum(
        "pcj,jg->pcg", filter_spectrum.astype(BF16), pick, preferred_element_type=F32
    ).astype(BF16)
    ca = lax.ppermute(column[:, :HALF], "seq", [(32, 0)] + [(64 - i, i) for i in range(1, 32)])
    cb = lax.ppermute(column[:, HALF:], "seq", [(32, 63)] + [(i + 1, i) for i in range(32, 63)])
    slot = jnp.arange(TOK // 2, dtype=jnp.int32)
    freq = 256 * (slot // 128 % 4) + 2 * (slot % 128) + slot // 512
    step = jnp.arange(SHARE, dtype=jnp.int32)
    angle = (freq[None, :] * (64 * step[:, None] + place) % LENGTH).astype(F32) * (
        2.0 * math.pi / LENGTH
    )
    parity = 1.0 - 2.0 * (step % 2).astype(F32)
    beta = jnp.stack(
        [jnp.cos(angle), jnp.where(freq[None, :] == 0, -parity[:, None], jnp.sin(angle))]
    )
    half_row = jnp.arange(64, dtype=jnp.int32)[:, None]
    half_freq = 2 * jnp.arange(128, dtype=jnp.int32)[None, :] + half_row // 32
    turn = ((half_row % 32) * half_freq % 64).astype(F32) * (2.0 * math.pi / 64)
    alpha = jnp.stack([jnp.cos(turn), jnp.sin(turn)])
    table = call(table_kernel, shape((TOK // 2, TOK), BF16), "vv")(alpha, beta)
    send, normed, kept = call(
        forward_kernel,
        (
            shape((NSEQ, 2 * QUART, 128), BF16),
            shape((CH, TOK), BF16),
            pltpu.HBM((TOK // 2, TOK), BF16),
        ),
        "v" * 7,
        scratch=[pltpu.VMEM((2, CH, TOK // 2), BF16), pltpu.SemaphoreType.DMA(())],
        outs="vvh",
        mib=20,
    )(tokens, sums, *others, norm_gain, table)
    moved = lax.all_to_all(send, "seq", split_axis=0, concat_axis=0, tiled=True)
    skip_col, gain_col, st_in, mix_in_t, up_t = call(
        up_kernel,
        (
            shape((CH, 1), F32), shape((CH, 1), F32), shape((8, TC), F32), shape((CH, CH), BF16),
            shape((HID, CH), BF16),
        ),
        "vvvv",
        scratch=[pltpu.VMEM((CH, CH), F32), pltpu.VMEM((CH, HID), F32)],
    )(skip_weight, mlp_gain, mix_in, up_weight)
    moved, skip_col, gain_col, st_in, mix_in_t, up_t = lax.optimization_barrier(
        (moved, skip_col, gain_col, st_in, mix_in_t, up_t)
    )
    back = call(
        middle_kernel,
        shape((NSEQ, 2 * QUART, 128), BF16),
        "shvhvv",
        scratch=[
            pltpu.VMEM((NSEQ, 2 * QUART, 128), BF16),
            pltpu.VMEM((2, HALF, TOK), BF16),
            pltpu.VMEM((2, NSEQ, 32, 128), F32),
            pltpu.VMEM((16 * HALF, 256), BF16),
            pltpu.VMEM((16 * HALF, 128), F32),
            pltpu.VMEM((NSEQ, 32, 128), F32),
            pltpu.VMEM((NSEQ, 32, 128), F32),
            pltpu.VMEM((2, NSEQ, 8, 128), F32),
            pltpu.VMEM((2, NSEQ, 8, 128), F32),
            pltpu.SemaphoreType.DMA((2,)),
        ],
    )(flags, in_hbm(moved), own, in_hbm(got), ca, cb)
    back, down_weight, mix_out = lax.optimization_barrier((back, down_weight, mix_out))
    down_t, mix_out_t = call(
        down_kernel,
        (shape((CH, HID), BF16), shape((CH, CH), BF16)),
        "vv",
        scratch=[pltpu.VMEM((CH, CH), F32), pltpu.VMEM((HID, CH), F32)],
    )(down_weight, mix_out)
    home = lax.all_to_all(back, "seq", split_axis=0, concat_axis=0, tiled=True)
    home, down_t, mix_out_t = lax.optimization_barrier((home, down_t, mix_out_t))
    piece = (shape((CH, TC), BF16),) + (shape((ROWS, TC), BF16),) * 4
    small = [
        pltpu.VMEM((CH, TC), F32),
        pltpu.VMEM((8, TC), F32),
        pltpu.VMEM((TC // 2, TOK), BF16),
        pltpu.SemaphoreType.DMA((TC // 256,)),
    ]
    rest = (in_hbm(kept), tokens, normed, skip_col, gain_col, st_in, mix_in_t)
    values, res_a, *first_a = call(
        back_first_kernel, (shape((CH, TOK), BF16),) + piece, "svhvvvvvv",
        scratch=[pltpu.VMEM((CH, TOK), F32)] + small, mib=20,
    )(flags, home, *rest)
    arrived_a = [first_a[0]] + [swap(first_a[k], k) for k in (1, 2, 3)]
    res_b, *first_b = call(
        back_second_kernel, piece, "svhvvvvvv", scratch=small, mib=20
    )(flags, values, *rest)
    arrived_b = [first_b[0]] + [swap(first_b[k], k) for k in (1, 2, 3)]

    def mlp(arrived):
        lows = call(
            mlp_kernel,
            (shape((PIECE, TC), BF16),) * 4,
            "s" + "v" * 6,
            scratch=[pltpu.VMEM((CH, TC), F32), pltpu.VMEM((CH, TC), F32)],
        )(flags, *arrived, up_t, down_t)
        return [lows[0]] + [swap(lows[k], k) for k in (1, 2, 3)]

    back_home_a = mlp(arrived_a)
    back_home_b = mlp(arrived_b)
    early = call(
        final_first_kernel, shape((CH, TC), BF16), "s" + "v" * 6, scratch=[pltpu.VMEM((CH, TC), F32)],
    )(flags, *back_home_a, res_a, mix_out_t)
    return call(
        final_second_kernel, shape((CH, TOK), BF16), "s" + "v" * 7, scratch=[pltpu.VMEM((CH, TC), F32)],
    )(flags, *back_home_b, res_b, mix_out_t, early)


def solution(mesh):
    in_specs = (
        P("chan", "seq"),
        P(None, "chan", "seq"),
        P("chan"),
        P("chan"),
        P("chan"),
        P("chan", None),
        P("chan", None),
        P("chan", None),
        P("chan", None),
    )
    out_specs = P("chan", "seq")
    return jax.shard_map(shards, mesh=mesh, in_specs=in_specs, out_specs=out_specs, check_vma=False)
```

```python
import math

import jax
import jax.numpy as jnp
from jax import lax
from jax.experimental import pallas as pl
from jax.experimental.pallas import tpu as pltpu
from jax.sharding import PartitionSpec as P


D = 768
CH = 192
HALF = 96
QUART = 24
TOK = 2048
NSEQ = 64
SHARE = 32
LENGTH = TOK * NSEQ
HID = 768
PIECE = 48
CHUNKS = 2
TC = TOK // CHUNKS
F32 = jnp.float32
BF16 = jnp.bfloat16
ROOT_HALF = math.sqrt(0.5)
MIB = 1024 * 1024
ROWS = 56


def vm():
    return pl.BlockSpec(memory_space=pltpu.VMEM)


def sm():
    return pl.BlockSpec(memory_space=pltpu.SMEM)


def hb():
    return pl.BlockSpec(memory_space=pltpu.HBM)


def call(body, out_shape, kinds, scratch=(), mib=14, outs=None):
    spec = {"s": sm, "v": vm, "h": hb}
    many = isinstance(out_shape, (tuple, list))
    outs = outs or "v" * (len(out_shape) if many else 1)
    return pl.pallas_call(
        body,
        out_shape=out_shape,
        in_specs=[spec[k]() for k in kinds],
        out_specs=[spec[k]() for k in outs] if many else spec[outs](),
        scratch_shapes=scratch,
        compiler_params=pltpu.CompilerParams(vmem_limit_bytes=mib * MIB),
    )


def in_hbm(x):
    return pltpu.with_memory_space_constraint(x, pltpu.HBM)


def shape(dims, dtype):
    return jax.ShapeDtypeStruct(dims, dtype)


def lane_group(rows):
    return lax.broadcasted_iota(jnp.int32, (rows, 128), 1)


def regroup(parts):
    lane = lane_group(parts[0].shape[0])
    step = list(parts)
    bit = len(parts) // 2
    while bit:
        d = 16 * bit
        low = (lane // d) % 2 == 0
        for a in range(len(parts)):
            if a & bit:
                continue
            x, y = step[a], step[a | bit]
            step[a] = jnp.where(low, x, pltpu.roll(y, d, 1))
            step[a | bit] = jnp.where(low, pltpu.roll(x, 128 - d, 1), y)
        bit //= 2
    return step


def column_of(row_ref):
    n = row_ref.shape[1]
    eye = lax.broadcasted_iota(jnp.int32, (n, n), 0) == lax.broadcasted_iota(jnp.int32, (n, n), 1)
    return jnp.sum(jnp.where(eye, row_ref[...], 0.0), axis=1, keepdims=True)


def sums_kernel(x_ref, out_ref):
    x = x_ref[...].astype(F32)
    out_ref[0:1, :] = jnp.sum(x, axis=0, keepdims=True)
    out_ref[1:2, :] = jnp.sum(x * x, axis=0, keepdims=True)


def give_kernel(flags, filter_ref, give_ref, held, sems):
    theirs = pl.multiple_of((1 - flags[0]) * HALF, HALF)
    rows = 32
    fetches = []
    for n in range(6):
        part, k = n // 3, n % 3
        fetches.append(
            pltpu.make_async_copy(
                filter_ref.at[part, pl.ds(theirs + rows * k, rows), :], held.at[n], sems.at[n]
            )
        )
        fetches[-1].start()
    for n in range(6):
        part, k = n // 3, n % 3
        fetches[n].wait()
        give_ref[part, rows * k : rows * (k + 1), :] = held[n].astype(BF16)


def table_kernel(alpha_ref, beta_ref, w_ref):
    def rows(b, carry):
        start = pl.multiple_of(b * SHARE, SHARE)
        for par in range(2):
            ac = jnp.broadcast_to(alpha_ref[0, pl.ds(b + 32 * par, 1), :], (SHARE, 128))
            as_ = jnp.broadcast_to(alpha_ref[1, pl.ds(b + 32 * par, 1), :], (SHARE, 128))
            for u in range(4 * par, 4 * par + 4):
                bc = beta_ref[0, :, 128 * u : 128 * (u + 1)]
                bs = beta_ref[1, :, 128 * u : 128 * (u + 1)]
                w_ref[pl.ds(start, SHARE), 256 * u : 256 * u + 128] = (ac * bc - as_ * bs).astype(
                    BF16
                )
                w_ref[pl.ds(start, SHARE), 256 * u + 128 : 256 * (u + 1)] = (
                    -(as_ * bc + ac * bs)
                ).astype(BF16)
        return carry

    lax.fori_loop(0, 32, rows, 0)


def forward_kernel(
    x_ref, s0, s1, s2, s3, gain_ref, w_ref, send_ref, normed_ref, kept_ref, fold, sem
):
    keep = pltpu.make_async_copy(w_ref, kept_ref, sem)
    keep.start()
    total = s0[...] + s1[...] + s2[...] + s3[...]
    mean = total[0:1, :] / D
    square = total[1:2, :] / D
    scale = lax.rsqrt(square - mean * mean + 1e-05)
    xn = ((x_ref[...].astype(F32) - mean) * scale * column_of(gain_ref)).astype(BF16)
    normed_ref[...] = xn
    left = xn[:, : TOK // 2].astype(F32)
    right = xn[:, TOK // 2 :].astype(F32)
    fold[0] = (left + right).astype(BF16)
    fold[1] = (left - right).astype(BF16)
    for b in range(4):
        y = [
            jnp.dot(
                fold[par],
                w_ref[:, 1024 * par + 256 * b : 1024 * par + 256 * (b + 1)],
                preferred_element_type=F32,
            )
            for par in range(2)
        ]
        for half in range(2):
            both = []
            for part in range(2):
                both.append(
                    regroup(
                        [
                            y[par][
                                half * HALF + w * QUART : half * HALF + (w + 1) * QUART,
                                128 * part : 128 * (part + 1),
                            ]
                            for par in range(2)
                            for w in range(4)
                        ]
                    )
                )
            for v in range(8):
                q = 8 * b + v
                dest = 63 - q if half else q
                send_ref[dest] = jnp.concatenate([both[0][v], both[1][v]], axis=0).astype(BF16)
    keep.wait()


def lanes_of(rows):
    lane = lax.broadcasted_iota(jnp.int32, (rows, 128), 1)
    group = (lane // 16) % 4
    return 2 * (lane % 16) + lane // 64, group


def make_gains(flags, own_ref, got_ref, ca_ref, cb_ref, g_ref, lhs, prod):
    high = flags[0] == 1
    first = flags[1] == 1
    row = lax.broadcasted_iota(jnp.int32, (128, 128), 0)
    freq, group = lanes_of(128)
    lane = SHARE * group + freq
    straight = jnp.where(row == lane, 1.0, 0.0)
    mirror = jnp.where((row + lane == 128) & (freq != 0), 1.0, 0.0)
    crow = lax.broadcasted_iota(jnp.int32, (NSEQ, 128), 0)
    cfreq, cgroup = lanes_of(NSEQ)
    keep = jnp.where(first, 0.0, 1.0)

    def column(part):
        return (ca_ref[part].astype(F32) + cb_ref[part].astype(F32)).astype(BF16)

    for part in range(2):
        sign = 1.0 if part == 0 else -1.0
        maps = jnp.concatenate([straight, sign * mirror], axis=0).astype(BF16)
        crossed = jnp.concatenate(
            [
                jnp.where((cfreq == 0) & (crow == 63 - 4 * t - cgroup), sign * keep, 0.0)
                for t in range(16)
            ],
            axis=1,
        ).astype(BF16)
        extra = jnp.dot(column(part), crossed, preferred_element_type=F32)
        own = own_ref[part]
        got = got_ref[part]
        direct = jnp.where(high, got, own)
        other = jnp.where(high, own, got)
        for t in range(16):
            rows = slice(HALF * t, HALF * (t + 1))
            lhs[rows, 0:128] = direct[:, 128 * t : 128 * (t + 1)]
            lhs[rows, 128:256] = other[:, 128 * (15 - t) : 128 * (16 - t)]
        prod[...] = jnp.dot(lhs[...], maps, preferred_element_type=F32)
        for t in range(16):
            out = regroup(
                [
                    prod[HALF * t + w * QUART : HALF * t + (w + 1) * QUART, :]
                    + extra[w * QUART : (w + 1) * QUART, 128 * t : 128 * (t + 1)]
                    for w in range(4)
                ]
            )
            for v in range(4):
                g_ref[part, 4 * t + v, 0:QUART, :] = out[v]

    @pl.when(first)
    def _():
        wide = [ca_ref[part].astype(F32) + cb_ref[part].astype(F32) for part in range(2)]
        alone = None
        for k in range(3):
            plain = jnp.concatenate(
                [
                    jnp.where((cfreq == 2 * k) & (crow == 4 * t + cgroup), 1.0, 0.0)
                    for t in range(16)
                ],
                axis=1,
            ).astype(BF16)
            rows = jnp.concatenate(
                [
                    wide[part][w * QUART + 8 * k : w * QUART + 8 * k + 8]
                    for part in range(2)
                    for w in range(4)
                ],
                axis=0,
            ).astype(BF16)
            more = jnp.dot(rows, plain, preferred_element_type=F32)
            alone = more if alone is None else alone + more
        for part in range(2):
            for t in range(16):
                out = regroup(
                    [
                        alone[32 * part + 8 * w : 32 * part + 8 * w + 8, 128 * t : 128 * (t + 1)]
                        for w in range(4)
                    ]
                )
                for v in range(4):
                    g_ref[part, 4 * t + v, QUART:32, :] = out[v]


def packed(tiles):
    return tiles[0] + pltpu.roll(tiles[1], 1, 1) + pltpu.roll(tiles[2], 2, 1)


def turn_i(re, im, s):
    return (-im, re) if s > 0 else (im, -re)


def dft4(xr, xi, s):
    ar, ai = xr[0] + xr[2], xi[0] + xi[2]
    br, bi = xr[0] - xr[2], xi[0] - xi[2]
    cr, ci = xr[1] + xr[3], xi[1] + xi[3]
    dr, di = turn_i(xr[1] - xr[3], xi[1] - xi[3], s)
    return [ar + cr, br + dr, ar - cr, br - dr], [ai + ci, bi + di, ai - ci, bi - di]


def dft8(xr, xi, s):
    er, ei = dft4(xr[0::2], xi[0::2], s)
    dr, di = dft4(xr[1::2], xi[1::2], s)
    c = ROOT_HALF
    if s > 0:
        dr1, di1 = c * (dr[1] - di[1]), c * (di[1] + dr[1])
        dr3, di3 = -c * (dr[3] + di[3]), c * (dr[3] - di[3])
    else:
        dr1, di1 = c * (dr[1] + di[1]), c * (di[1] - dr[1])
        dr3, di3 = c * (di[3] - dr[3]), -c * (di[3] + dr[3])
    dr2, di2 = turn_i(dr[2], di[2], s)
    qr = [dr[0], dr1, dr2, dr3]
    qi = [di[0], di1, di2, di3]
    return (
        [er[k] + qr[k] for k in range(4)] + [er[k] - qr[k] for k in range(4)],
        [ei[k] + qi[k] for k in range(4)] + [ei[k] - qi[k] for k in range(4)],
    )


def twiddle(re, im, index, s):
    index %= 64
    if index == 0:
        return re, im
    c = math.cos(2.0 * math.pi * index / 64.0)
    d = s * math.sin(2.0 * math.pi * index / 64.0)
    return re * c - im * d, im * c + re * d


def across(load, store, gains, a_ref, b_ref):
    for p0 in range(8):
        xr, xi = zip(*[load(p0 + 8 * p1) for p1 in range(8)])
        yr, yi = dft8(list(xr), list(xi), -1)
        for g1 in range(8):
            a_ref[0, g1 * 8 + p0], a_ref[1, g1 * 8 + p0] = twiddle(yr[g1], yi[g1], p0 * g1, -1)
    for g1 in range(8):
        yr, yi = dft8(
            [a_ref[0, g1 * 8 + p0] for p0 in range(8)],
            [a_ref[1, g1 * 8 + p0] for p0 in range(8)],
            -1,
        )
        for g2 in range(8):
            hr, hi = gains(g1 + 8 * g2)
            yr[g2], yi[g2] = hr * yr[g2] - hi * yi[g2], hr * yi[g2] + hi * yr[g2]
        zr, zi = dft8(yr, yi, 1)
        for p0 in range(8):
            b_ref[0, p0 * 8 + g1], b_ref[1, p0 * 8 + g1] = twiddle(zr[p0], zi[p0], g1 * p0, 1)
    for p0 in range(8):
        zr, zi = dft8(
            [b_ref[0, p0 * 8 + g1] for g1 in range(8)],
            [b_ref[1, p0 * 8 + g1] for g1 in range(8)],
            1,
        )
        for p1 in range(8):
            store(p0 + 8 * p1, zr[p1], zi[p1])


def middle_kernel(
    flags, moved, own_ref, got, ca_ref, cb_ref, out_ref,
    moved_ref, got_ref, g_ref, lhs, prod, xr_ref, xi_ref, a_ref, b_ref, sems,
):
    first = flags[1] == 1
    fetches = [
        pltpu.make_async_copy(got, got_ref, sems.at[0]),
        pltpu.make_async_copy(moved, moved_ref, sems.at[1]),
    ]
    for fetch in fetches:
        fetch.start()
    freq, _ = lanes_of(QUART)
    special = (freq == 0) & first
    fetches[0].wait()
    make_gains(flags, own_ref, got_ref, ca_ref, cb_ref, g_ref, lhs, prod)
    fetches[1].wait()

    def widen(p, carry):
        both = moved_ref[p].astype(F32)
        xr_ref[p, 0:QUART, :] = both[:QUART]
        xi_ref[p, 0:QUART, :] = jnp.where(special, 0.0, both[QUART:])
        return carry

    lax.fori_loop(0, NSEQ, widen, 0, unroll=8)

    def half_turn(p):
        return math.cos(2.0 * math.pi * p / 128.0), math.sin(2.0 * math.pi * p / 128.0)

    @pl.when(first)
    def _():
        for p in range(NSEQ):
            c, s = half_turn(p)
            im = jnp.where(special, moved_ref[p].astype(F32)[QUART:], 0.0)
            im = packed([im[8 * k : 8 * k + 8] for k in range(3)])
            xr_ref[p, QUART:32, :] = im * c
            xi_ref[p, QUART:32, :] = im * (-s)

    def every(i, carry):
        rows = pl.ds(pl.multiple_of(i * 8, 8), 8)

        def load(p):
            return xr_ref[p, rows, :], xi_ref[p, rows, :]

        def store(p, re, im):
            xr_ref[p, rows, :] = re
            xi_ref[p, rows, :] = im

        across(load, store, lambda g: (g_ref[0, g, rows, :], g_ref[1, g, rows, :]), a_ref, b_ref)
        return carry

    lax.fori_loop(0, 3 + flags[1], every, 0)

    @pl.when(first)
    def _():
        for p in range(NSEQ):
            c, s = half_turn(p)
            one = xr_ref[p, QUART:32, :] * c - xi_ref[p, QUART:32, :] * s
            alone = jnp.concatenate([one, pltpu.roll(one, 127, 1), pltpu.roll(one, 126, 1)], axis=0)
            xi_ref[p, 0:QUART, :] = jnp.where(special, alone, xi_ref[p, 0:QUART, :])

    def narrow(p, carry):
        out_ref[p] = jnp.concatenate(
            [xr_ref[p, 0:QUART, :], xi_ref[p, 0:QUART, :]], axis=0
        ).astype(BF16)
        return carry

    lax.fori_loop(0, NSEQ, narrow, 0, unroll=8)


def in_three(x):
    a = x.astype(BF16)
    rest = x - a.astype(F32)
    b = rest.astype(BF16)
    return [a, b, (rest - b.astype(F32)).astype(BF16)]


def tokens_back(
    flags, values, w_ref, x_ref, normed_ref, skip, gain, st_in, mix_t_ref, res_ref, outs, tm, st,
    fetches,
    chunk,
):
    me = flags[2]
    skip = skip[...]
    gain = gain[...]
    st[...] = st_in[...]
    for n in range(TC // 512):
        mine = slice(256 * n, 256 * (n + 1))
        fetches[n].wait()
        sums = []
        for par in range(2):
            sums.append(
                lax.dot_general(
                    values[:, 1024 * par : 1024 * (par + 1)],
                    w_ref[mine, 1024 * par : 1024 * (par + 1)],
                    (((1,), (1,)), ((), ())),
                    preferred_element_type=F32,
                )
            )
        even, odd = sums
        for side, conv in enumerate((even + odd, even - odd)):
            here = slice(side * TC // 2 + 256 * n, side * TC // 2 + 256 * (n + 1))
            start = side * TOK // 2 + chunk * TC // 2 + 256 * n
            cols = slice(start, start + 256)
            res = (
                x_ref[:, cols].astype(F32)
                + conv * (1.0 / LENGTH)
                + skip * normed_ref[:, cols].astype(F32)
            ).astype(BF16)
            res_ref[:, here] = res
            r = res.astype(F32)
            mean = jnp.sum(r, axis=0, keepdims=True) * (1.0 / CH)
            centred = r - mean
            for k, part in enumerate(in_three(mean)):
                st[k : k + 1, here] = part.astype(F32)
            for k, part in enumerate(
                in_three(jnp.sum(centred * centred, axis=0, keepdims=True))[:2]
            ):
                st[3 + k : 4 + k, here] = part.astype(F32)
            z = (centred * gain).astype(BF16)
            tm[:, here] = jnp.dot(mix_t_ref[...], z, preferred_element_type=F32)
    for k in range(4):
        rows = pl.ds(pl.multiple_of((me ^ k) * PIECE, PIECE), PIECE)
        outs[k][...] = jnp.concatenate([tm[rows, :], st[...]], axis=0).astype(BF16)


def fetch_table(w_hbm, w_ref, sems, chunk):
    fetches = []
    for n in range(TC // 512):
        here = slice(256 * n, 256 * (n + 1))
        there = slice(chunk * TC // 2 + 256 * n, chunk * TC // 2 + 256 * (n + 1))
        fetches.append(pltpu.make_async_copy(w_hbm.at[there, :], w_ref.at[here, :], sems.at[n]))
        fetches[-1].start()
    return fetches


def back_first_kernel(
    flags, got_ref, w_hbm, x_ref, normed_ref, skip_ref, gain_ref, st_in, mix_t_ref,
    values_ref, res_ref, u0, u1, u2, u3, tall, tm, st, w_ref, sems,
):
    fetches = fetch_table(w_hbm, w_ref, sems, 0)
    for half in range(2):
        for b in range(4):
            parts = []
            for v in range(8):
                q = 8 * b + v
                parts.append(got_ref[63 - q if half else q].astype(F32))
            out = regroup(parts)
            for k in range(8):
                low = half * HALF + (k % 4) * QUART
                left = 1024 * (k // 4) + 256 * b
                tall[low : low + QUART, left : left + 128] = out[k][:QUART]
                tall[low : low + QUART, left + 128 : left + 256] = out[k][QUART:]
    values = tall[...].astype(BF16)
    values_ref[...] = values
    tokens_back(
        flags, values_ref[...], w_ref, x_ref, normed_ref, skip_ref, gain_ref, st_in, mix_t_ref, res_ref,
        (u0, u1, u2, u3), tm, st, fetches, 0,
    )


def back_second_kernel(
    flags, values_ref, w_hbm, x_ref, normed_ref, skip_ref, gain_ref, st_in, mix_t_ref,
    res_ref, u0, u1, u2, u3, tm, st, w_ref, sems,
):
    fetches = fetch_table(w_hbm, w_ref, sems, 1)
    tokens_back(
        flags, values_ref[...], w_ref, x_ref, normed_ref, skip_ref, gain_ref, st_in, mix_t_ref, res_ref,
        (u0, u1, u2, u3), tm, st, fetches, 1,
    )


def mlp_kernel(flags, p0, p1, p2, p3, up_t, down_t, o0, o1, o2, o3, f_ref, low_ref):
    me = flags[2]
    values = [p[...].astype(F32) for p in (p0, p1, p2, p3)]
    tails = [x[PIECE:ROWS] for x in values]
    means = [t[0:1] + t[1:2] + t[2:3] for t in tails]
    mean = (means[0] + means[1] + means[2] + means[3]) * 0.25
    spread = sum(t[3:4] + t[4:5] for t in tails) + CH * sum((m - mean) * (m - mean) for m in means)
    scale = lax.rsqrt(spread * (1.0 / D) + 1e-05)
    row = lax.broadcasted_iota(jnp.int32, (PIECE, CH), 0)
    lane = lax.broadcasted_iota(jnp.int32, (PIECE, CH), 1)
    pick = lane == row + me * PIECE
    for k in range(4):
        line = tails[k][5:6, 0:CH] + tails[k][6:7, 0:CH]
        weight = jnp.sum(jnp.where(pick, line, 0.0), axis=1, keepdims=True)
        f_ref[pl.ds(pl.multiple_of((me ^ k) * PIECE, PIECE), PIECE), :] = scale * (
            values[k][:PIECE] - (mean - means[k]) * weight
        )
    for n in range(TC // 256):
        cols = slice(256 * n, 256 * (n + 1))
        f = f_ref[:, cols].astype(BF16)
        total = None
        for h in range(3):
            rows = slice(256 * h, 256 * (h + 1))
            wide = jnp.dot(up_t[rows, :], f, preferred_element_type=F32)
            act = (0.5 * wide * (1.0 + lax.erf(wide * ROOT_HALF))).astype(BF16)
            part = jnp.dot(down_t[:, rows], act, preferred_element_type=F32)
            total = part if total is None else total + part
        low_ref[:, cols] = total
    for k, o in enumerate((o0, o1, o2, o3)):
        o[...] = low_ref[pl.ds(pl.multiple_of((me ^ k) * PIECE, PIECE), PIECE), :].astype(BF16)


def unroll(src, dst, rows, cols):
    def step(i, carry):
        for k in range(8):
            row = i * 8 + k
            start = pl.multiple_of(row * cols, 128)
            dst[pl.ds(row, 1), :] = src[:, pl.ds(start, cols)].astype(F32)
        return carry

    lax.fori_loop(0, rows // 8, step, 0)


def up_kernel(
    skip_row, gain_row, mix_in_ref, up_ref, skip_ref, gain_ref, st_ref, in_t, up_t, square, wide, tall
):
    skip_ref[...] = column_of(skip_row)
    gain_ref[...] = column_of(gain_row)
    unroll(up_ref, wide, CH, HID)
    turned = wide[...].T
    tall[0] = turned[:, 0:128]
    tall[1, :, 0 : CH - 128] = turned[:, 128:CH]
    for par in range(2):
        rows = slice(par * HID // 2, (par + 1) * HID // 2)
        picked = [tall[k, pl.ds(par, HID // 2, stride=2), :] for k in range(2)]
        up_t[rows, 0:128] = picked[0].astype(BF16)
        up_t[rows, 128:CH] = picked[1][:, 0 : CH - 128].astype(BF16)
    paired(mix_in_ref, square, CH)
    in_t[...] = square[...].T.astype(BF16)
    st_ref[...] = jnp.zeros((8, TC), F32)
    weight = jnp.dot(
        gain_row[...], square[...], preferred_element_type=F32, precision=lax.Precision.HIGHEST
    )
    for k, part in enumerate(in_three(weight)[:2]):
        st_ref[5 + k : 6 + k, 0:CH] = part.astype(F32)


def down_kernel(down_ref, mix_out_ref, down_t, out_t, square, pairs):
    paired(mix_out_ref, square, CH)
    out_t[...] = square[...].T.astype(BF16)
    unroll(down_ref, pairs, HID // 2, 2 * CH)
    both = pairs[...]
    for par in range(2):
        down_t[:, par * HID // 2 : (par + 1) * HID // 2] = both[:, par * CH : (par + 1) * CH].T.astype(
            BF16
        )


def paired(src, dst, rows):
    def step(i, carry):
        for k in range(4):
            row = i * 8 + 2 * k
            start = pl.multiple_of(row * CH, 128)
            both = src[:, pl.ds(start, 2 * CH)].astype(F32)
            dst[pl.ds(row, 1), :] = both[:, :CH]
            dst[pl.ds(row + 1, 1), :] = both[:, CH:]
        return carry

    lax.fori_loop(0, rows // 8, step, 0)


def tokens_out(flags, pieces, res_ref, mix_t_ref, f_ref, store):
    me = flags[2]
    for k in range(4):
        rows = pl.ds(pl.multiple_of((me ^ k) * PIECE, PIECE), PIECE)
        f_ref[rows, :] = pieces[k][...].astype(F32)
    for n in range(TC // 256):
        cols = slice(256 * n, 256 * (n + 1))
        add = jnp.dot(mix_t_ref[...], f_ref[:, cols].astype(BF16), preferred_element_type=F32)
        store(cols, (res_ref[:, cols].astype(F32) + add).astype(BF16))


def final_first_kernel(flags, p0, p1, p2, p3, res_ref, mix_t_ref, out_ref, f_ref):
    def store(cols, x):
        out_ref[:, cols] = x

    tokens_out(flags, (p0, p1, p2, p3), res_ref, mix_t_ref, f_ref, store)


def final_second_kernel(flags, p0, p1, p2, p3, res_ref, mix_t_ref, early_ref, out_ref, f_ref):
    side = TC // 2
    for k in range(2):
        out_ref[:, 2 * k * side : (2 * k + 1) * side] = early_ref[:, k * side : (k + 1) * side]

    def store(cols, x):
        start = cols.start + (side if cols.start < side else 2 * side)
        out_ref[:, start : start + 256] = x

    tokens_out(flags, (p0, p1, p2, p3), res_ref, mix_t_ref, f_ref, store)


def swap(x, k):
    return lax.ppermute(x, "chan", [(i, i ^ k) for i in range(4)])


def shards(
    tokens, filter_spectrum, skip_weight, norm_gain, mlp_gain, mix_in, up_weight, down_weight, mix_out
):
    return block(
        tokens, filter_spectrum, skip_weight[None], norm_gain[None], mlp_gain[None], mix_in,
        up_weight, down_weight, mix_out,
    )


def block(
    tokens, filter_spectrum, skip_weight, norm_gain, mlp_gain, mix_in, up_weight, down_weight, mix_out
):
    place = lax.axis_index("seq")
    lane_of = lax.axis_index("chan")
    high = place >= 32
    first = (place == 0) | (place == 63)
    flags = jnp.stack([high, first, lane_of, place]).astype(jnp.int32)
    mine = jnp.where(high, HALF, 0)
    give = call(
        give_kernel, shape((2, HALF, TOK), BF16), "sh",
        scratch=[pltpu.VMEM((6, 32, TOK), F32), pltpu.SemaphoreType.DMA((6,))],
    )(flags, in_hbm(filter_spectrum))
    got = lax.ppermute(give, "seq", [(i, 63 - i) for i in range(64)])
    sums = call(sums_kernel, shape((2, TOK), F32), "v")(tokens)
    others = []
    for k in (1, 2, 3):
        others.append(swap(sums, k))
    own = lax.dynamic_slice_in_dim(filter_spectrum, mine, HALF, 1).astype(BF16)
    pick_row = jnp.arange(TOK, dtype=jnp.int32)[:, None]
    pick_col = jnp.arange(NSEQ, dtype=jnp.int32)[None, :]
    pick = (pick_row == SHARE * pick_col).astype(BF16)
    column = jnp.einsum(
        "pcj,jg->pcg", filter_spectrum.astype(BF16), pick, preferred_element_type=F32
    ).astype(BF16)
    ca = lax.ppermute(column[:, :HALF], "seq", [(32, 0)] + [(64 - i, i) for i in range(1, 32)])
    cb = lax.ppermute(column[:, HALF:], "seq", [(32, 63)] + [(i + 1, i) for i in range(32, 63)])
    slot = jnp.arange(TOK // 2, dtype=jnp.int32)
    freq = 256 * (slot // 128 % 4) + 2 * (slot % 128) + slot // 512
    step = jnp.arange(SHARE, dtype=jnp.int32)
    angle = (freq[None, :] * (64 * step[:, None] + place) % LENGTH).astype(F32) * (
        2.0 * math.pi / LENGTH
    )
    parity = 1.0 - 2.0 * (step % 2).astype(F32)
    beta = jnp.stack(
        [jnp.cos(angle), jnp.where(freq[None, :] == 0, -parity[:, None], jnp.sin(angle))]
    )
    half_row = jnp.arange(64, dtype=jnp.int32)[:, None]
    half_freq = 2 * jnp.arange(128, dtype=jnp.int32)[None, :] + half_row // 32
    turn = ((half_row % 32) * half_freq % 64).astype(F32) * (2.0 * math.pi / 64)
    alpha = jnp.stack([jnp.cos(turn), jnp.sin(turn)])
    table = call(table_kernel, shape((TOK // 2, TOK), BF16), "vv")(alpha, beta)
    send, normed, kept = call(
        forward_kernel,
        (
            shape((NSEQ, 2 * QUART, 128), BF16),
            shape((CH, TOK), BF16),
            pltpu.HBM((TOK // 2, TOK), BF16),
        ),
        "v" * 7,
        scratch=[pltpu.VMEM((2, CH, TOK // 2), BF16), pltpu.SemaphoreType.DMA(())],
        outs="vvh",
        mib=20,
    )(tokens, sums, *others, norm_gain, table)
    moved = lax.all_to_all(send, "seq", split_axis=0, concat_axis=0, tiled=True)
    skip_col, gain_col, st_in, mix_in_t, up_t = call(
        up_kernel,
        (
            shape((CH, 1), F32), shape((CH, 1), F32), shape((8, TC), F32), shape((CH, CH), BF16),
            shape((HID, CH), BF16),
        ),
        "vvvv",
        scratch=[
            pltpu.VMEM((CH, CH), F32), pltpu.VMEM((CH, HID), F32), pltpu.VMEM((2, HID, 128), F32)
        ],
    )(skip_weight, mlp_gain, mix_in, up_weight)
    moved, skip_col, gain_col, st_in, mix_in_t, up_t = lax.optimization_barrier(
        (moved, skip_col, gain_col, st_in, mix_in_t, up_t)
    )
    back = call(
        middle_kernel,
        shape((NSEQ, 2 * QUART, 128), BF16),
        "shvhvv",
        scratch=[
            pltpu.VMEM((NSEQ, 2 * QUART, 128), BF16),
            pltpu.VMEM((2, HALF, TOK), BF16),
            pltpu.VMEM((2, NSEQ, 32, 128), F32),
            pltpu.VMEM((16 * HALF, 256), BF16),
            pltpu.VMEM((16 * HALF, 128), F32),
            pltpu.VMEM((NSEQ, 32, 128), F32),
            pltpu.VMEM((NSEQ, 32, 128), F32),
            pltpu.VMEM((2, NSEQ, 8, 128), F32),
            pltpu.VMEM((2, NSEQ, 8, 128), F32),
            pltpu.SemaphoreType.DMA((2,)),
        ],
    )(flags, in_hbm(moved), own, in_hbm(got), ca, cb)
    back, down_weight, mix_out = lax.optimization_barrier((back, down_weight, mix_out))
    down_t, mix_out_t = call(
        down_kernel,
        (shape((CH, HID), BF16), shape((CH, CH), BF16)),
        "vv",
        scratch=[pltpu.VMEM((CH, CH), F32), pltpu.VMEM((HID // 2, 2 * CH), F32)],
    )(down_weight, mix_out)
    home = lax.all_to_all(back, "seq", split_axis=0, concat_axis=0, tiled=True)
    home, down_t, mix_out_t = lax.optimization_barrier((home, down_t, mix_out_t))
    piece = (shape((CH, TC), BF16),) + (shape((ROWS, TC), BF16),) * 4
    small = [
        pltpu.VMEM((CH, TC), F32),
        pltpu.VMEM((8, TC), F32),
        pltpu.VMEM((TC // 2, TOK), BF16),
        pltpu.SemaphoreType.DMA((TC // 512,)),
    ]
    rest = (in_hbm(kept), tokens, normed, skip_col, gain_col, st_in, mix_in_t)
    values, res_a, *first_a = call(
        back_first_kernel, (shape((CH, TOK), BF16),) + piece, "svhvvvvvv",
        scratch=[pltpu.VMEM((CH, TOK), F32)] + small, mib=20,
    )(flags, home, *rest)
    arrived_a = [first_a[0]] + [swap(first_a[k], k) for k in (1, 2, 3)]
    res_b, *first_b = call(
        back_second_kernel, piece, "svhvvvvvv", scratch=small, mib=20
    )(flags, values, *rest)
    arrived_b = [first_b[0]] + [swap(first_b[k], k) for k in (1, 2, 3)]

    def mlp(arrived):
        lows = call(
            mlp_kernel,
            (shape((PIECE, TC), BF16),) * 4,
            "s" + "v" * 6,
            scratch=[pltpu.VMEM((CH, TC), F32), pltpu.VMEM((CH, TC), F32)],
        )(flags, *arrived, up_t, down_t)
        return [lows[0]] + [swap(lows[k], k) for k in (1, 2, 3)]

    back_home_a = mlp(arrived_a)
    back_home_b = mlp(arrived_b)
    early = call(
        final_first_kernel, shape((CH, TC), BF16), "s" + "v" * 6, scratch=[pltpu.VMEM((CH, TC), F32)],
    )(flags, *back_home_a, res_a, mix_out_t)
    return call(
        final_second_kernel, shape((CH, TOK), BF16), "s" + "v" * 7, scratch=[pltpu.VMEM((CH, TC), F32)],
    )(flags, *back_home_b, res_b, mix_out_t, early)


def solution(mesh):
    in_specs = (
        P("chan", "seq"),
        P(None, "chan", "seq"),
        P("chan"),
        P("chan"),
        P("chan"),
        P("chan", None),
        P("chan", None),
        P("chan", None),
        P("chan", None),
    )
    out_specs = P("chan", "seq")
    return jax.shard_map(shards, mesh=mesh, in_specs=in_specs, out_specs=out_specs, check_vma=False)
```
